32 devices in a mesh: seq: 8 (over y, x, core), ad: 4 (over z).
Axes of the slice: x: 2, y: 2, z: 4, core: 2. Of those that a mesh axis runs over, the one named last changes fastest.
Arguments:
- tokens: bfloat16 [4, 2048, 2048], P('ad', 'seq'), may hold values from -6 to 6
- out_grad: bfloat16 [4, 2048, 2048], P('ad', 'seq'), may hold values from -6 to 6
- block_role: int32 [4, 16], P('ad'), may hold values from 0 to 15, each once within a row
- adapter_of: int32 [4, 8], P('ad'), may hold values from 0 to 7
- attn_gain: float32 [2048], replicated, may hold values from 0.1 to 1.9
- ffn_gain: float32 [2048], replicated, may hold values from 0.1 to 1.9
- wqkv: bfloat16 [2048, 4096], P(('seq', 'ad')), may hold values from -0.125 to 0.125
- wo: bfloat16 [2048, 2048], P(('seq', 'ad')), may hold values from -0.5 to 0.5
- ffn: bfloat16 [2048, 3, 8192], P(('seq', 'ad')), may hold values from -0.125 to 0.125
- qkv_a: bfloat16 [8, 16, 2048], P('ad'), may hold values from -0.125 to 0.125
- qkv_b: bfloat16 [8, 16, 4096], P('ad'), may hold values from -1.5 to 1.5
- out_a: bfloat16 [8, 16, 2048], P('ad'), may hold values from -0.5 to 0.5
- out_b: bfloat16 [8, 16, 2048], P('ad'), may hold values from -1.5 to 1.5
- ffn_in_a: bfloat16 [8, 2, 16, 2048], P('ad'), may hold values from -0.125 to 0.125
- ffn_in_b: bfloat16 [8, 2, 16, 8192], P('ad'), may hold values from -1.5 to 1.5
- ffn_out_a: bfloat16 [8, 16, 8192], P('ad'), may hold values from -0.0625 to 0.0625
- ffn_out_b: bfloat16 [8, 16, 2048], P('ad'), may hold values from -1.5 to 1.5
Outputs:
- output: bfloat16 [4, 2048, 2048], P('ad', 'seq')
- input_grad: float32 [4, 2048, 2048], P('ad', 'seq')
- qkv_a_grad: float32 [8, 16, 2048], P('ad')
- qkv_b_grad: float32 [8, 16, 4096], P('ad')
- out_a_grad: float32 [8, 16, 2048], P('ad')
- out_b_grad: float32 [8, 16, 2048], P('ad')
- ffn_in_a_grad: float32 [8, 2, 16, 2048], P('ad')
- ffn_in_b_grad: float32 [8, 2, 16, 8192], P('ad')
- ffn_out_a_grad: float32 [8, 16, 8192], P('ad')
- ffn_out_b_grad: float32 [8, 16, 2048], P('ad')
The draws below stay inside these ranges and needn't reach their ends.
Inputs may be any that keep to these rules, and one draw needn't show every extreme that they name: `block_role`: each group's row names every role once; roles below 8 are the prompt's blocks in order, the others continuations.
All inputs are finite; a program needn't handle non-finite values.
Results may differ from the reference program's by a relative error of at most 0.025.
Values may be sent and summed in bfloat16 or wider, within the bound.
A program may use at most 256 MiB of HBM per device.

```python
import math
import jax
import jax.numpy as jnp
from jax import lax

D = 2048
QUERY_HEADS = 16
KEY_VALUE_HEADS = 8
HEAD_SIZE = 128
FF = 8192
R = 16
NA = 8
PBLK = 8
CONTS = 8
BLOCK = 128
SLOTS = 16
GTOK = 2048
GROUPS = 4
QKV = 4096


def touch_ends(entries, stream_key, low, largest):
    longest = entries.shape.index(max(entries.shape))
    spots = []
    for shift in (0, 1):
        where = [jax.random.randint(jax.random.fold_in(stream_key, axis), (), 0, length) for axis, length in enumerate(entries.shape)]
        where[longest] = (where[longest] + shift) % entries.shape[longest]
        spots.append(tuple(where))
    return entries.at[spots[0]].set(low).at[spots[1]].set(largest)


def shard_levels(key, dims, pieces, least, high):
    loudness = 1.0
    for axis_at, blocks in pieces:
        heights = jax.random.uniform(jax.random.fold_in(jax.random.fold_in(key, 6), axis_at), (blocks,), jnp.float32, least / len(pieces), high / len(pieces))
        loudness = loudness * jnp.repeat(jnp.exp(heights), dims[axis_at] // blocks).reshape((-1,) + (1,) * (len(dims) - 1 - axis_at))
    return loudness


def noise(rng, shape, spread, reach, cuts=(), kind=jnp.bfloat16):
    entries = jax.random.normal(rng, shape, jnp.float32) * spread
    if len(cuts) > 0:
        entries = shard_levels(rng, shape, cuts, -0.22, 0.18) * entries
    return jnp.clip(entries, min=-reach, max=reach).astype(kind)


def setup_inputs(seed: int = 0) -> dict:
    streams_of = jax.random.split(jax.random.key(seed), 18)
    tokens = noise(streams_of[0], (GROUPS, GTOK, D), 1.0, 6.0, ((0, 4), (1, 8)))
    out_grad = noise(streams_of[1], (GROUPS, GTOK, D), 1.0, 6.0, ((0, 4), (1, 8)))
    block_role = jax.vmap(lambda own: jax.random.permutation(own, SLOTS))(jax.random.split(streams_of[2], GROUPS)).reshape((GROUPS, SLOTS)).astype(jnp.int32)
    adapter_of = touch_ends(jax.random.randint(streams_of[3], (GROUPS, CONTS), 0, NA), jax.random.fold_in(streams_of[3], 1), 0, NA - 1).astype(jnp.int32)
    attn_gain = jnp.clip(1.0 + 0.18 * jax.random.normal(streams_of[4], (D,), jnp.float32), 0.1, 1.9)
    ffn_gain = jnp.clip(1.0 + 0.18 * jax.random.normal(streams_of[5], (D,), jnp.float32), 0.1, 1.9)
    wqkv = noise(streams_of[6], (D, QKV), D ** -0.5, 0.125, ((0, 32),))
    wo = noise(streams_of[7], (QUERY_HEADS * HEAD_SIZE, D), (QUERY_HEADS * HEAD_SIZE // 16) ** -0.5, 0.5, ((0, 32),))
    ffn = noise(streams_of[8], (D, 3, FF), D ** -0.5, 0.125, ((0, 32),))
    qkv_a = noise(streams_of[9], (NA, R, D), D ** -0.5, 0.125, ((0, 4),))
    qkv_b = noise(streams_of[10], (NA, R, QKV), R ** -0.5, 1.5, ((0, 4),))
    out_a = noise(streams_of[11], (NA, R, QUERY_HEADS * HEAD_SIZE), (QUERY_HEADS * HEAD_SIZE // 16) ** -0.5, 0.5, ((0, 4),))
    out_b = noise(streams_of[12], (NA, R, D), R ** -0.5, 1.5, ((0, 4),))
    ffn_in_a = noise(streams_of[13], (NA, 2, R, D), D ** -0.5, 0.125, ((0, 4),))
    ffn_in_b = noise(streams_of[14], (NA, 2, R, FF), R ** -0.5, 1.5, ((0, 4),))
    ffn_out_a = noise(streams_of[15], (NA, R, FF), FF ** -0.5, 0.0625, ((0, 4),))
    ffn_out_b = noise(streams_of[16], (NA, R, D), R ** -0.5, 1.5, ((0, 4),))
    return {"tokens": tokens, "out_grad": out_grad, "block_role": block_role, "adapter_of": adapter_of, "attn_gain": attn_gain, "ffn_gain": ffn_gain, "wqkv": wqkv, "wo": wo, "ffn": ffn, "qkv_a": qkv_a, "qkv_b": qkv_b, "out_a": out_a, "out_b": out_b, "ffn_in_a": ffn_in_a, "ffn_in_b": ffn_in_b, "ffn_out_a": ffn_out_a, "ffn_out_b": ffn_out_b}


@jax.custom_vjp
def low_rank_part(v):
    return lax.optimization_barrier(v.astype(jnp.bfloat16)).astype(jnp.float32)

@jax.custom_vjp
def low_back(v):
    return v

def low_keep(v):
    return (low_rank_part(v), None)

def low_pass(kept, grad):
    return (grad,)

def back_keep(v):
    return (v, None)

def back_low(kept, grad):
    return (low_rank_part(grad),)
low_rank_part.defvjp(low_keep, low_pass)
low_back.defvjp(back_keep, back_low)
eps_norm = 1e-05
rope_base = 1000000.0

def highest(matrix_a, matrix_b):
    return jnp.dot(matrix_a, matrix_b, precision=lax.Precision.HIGHEST)

def stacked(matrix_a):
    return matrix_a.reshape(matrix_a.shape[0] * matrix_a.shape[1], matrix_a.shape[2])

def normalize(values, gain):
    return values * lax.rsqrt(lax.optimization_barrier(jnp.mean(values * values, axis=-1, keepdims=True)) + eps_norm) * gain

def rotary_tables(values, token_position):
    half_size = values.shape[-1] // 2
    frequency = jnp.exp(jnp.arange(half_size, dtype=jnp.float32) * (-2.0 * math.log(rope_base) / values.shape[-1]))
    angles = token_position.astype(jnp.float32)[:, None] * frequency[None, :]
    cosine = jnp.cos(angles)[:, None, :]
    sine_table = jnp.sin(angles)[:, None, :]
    leading = values[..., :half_size]
    trailing = values[..., half_size:]
    return jnp.concatenate([leading * cosine - trailing * sine_table, trailing * cosine + leading * sine_table], axis=-1)

def token_layout(role_row, owner_row):
    role_tok = jnp.repeat(role_row, BLOCK)
    offset = jnp.arange(SLOTS * BLOCK, dtype=jnp.int32) % BLOCK
    is_later = role_tok >= PBLK
    token_position = jnp.where(is_later, PBLK * BLOCK + offset, role_tok * BLOCK + offset)
    matches = (role_tok - PBLK)[:, None] == jnp.arange(CONTS, dtype=jnp.int32)[None, :]
    owner_tok = lax.optimization_barrier(jnp.max(jnp.where(matches, owner_row[None, :], -1), axis=1))
    column_owner = jnp.arange(NA * R, dtype=jnp.int32) // R
    select = (owner_tok[:, None] == column_owner[None, :]).astype(jnp.float32)
    return (role_tok, token_position, select)

def visible_mask(query_role, query_pos, key_role, key_pos):
    causal = key_pos[None, :] <= query_pos[:, None]
    prompt_key = (key_role[None, :] < PBLK) & ((query_role[:, None] >= PBLK) | causal)
    own_key = (key_role[None, :] >= PBLK) & (key_role[None, :] == query_role[:, None]) & causal
    return prompt_key | own_key

def group_forward(inputs_f, role_row, owner_row, stacks, weights):
    qkv_a, qkv_b, out_a, out_b, ffn_in_a, ffn_in_b, ffn_out_a, ffn_out_b = stacks
    attn_gain, ffn_gain, wqkv, wo, ffn = weights
    role_tok, token_position, select = token_layout(role_row, owner_row)
    visible = visible_mask(role_tok, token_position, role_tok, token_position)
    token_length = inputs_f.shape[0]
    heads_per_group = QUERY_HEADS // KEY_VALUE_HEADS
    score_scale = 1.0 / math.sqrt(HEAD_SIZE)
    normed_attn = low_rank_part(normalize(inputs_f, attn_gain))
    rank_qkv = low_back(low_rank_part(highest(normed_attn, stacked(qkv_a).T))) * select
    projected_rows = low_back(highest(normed_attn, wqkv) + highest(rank_qkv, stacked(qkv_b)))
    projected_rows = projected_rows.reshape(token_length, KEY_VALUE_HEADS, heads_per_group + 2, HEAD_SIZE)
    query_rows = low_rank_part(rotary_tables(projected_rows[:, :, :heads_per_group].reshape(token_length, QUERY_HEADS, HEAD_SIZE), token_position)).reshape(token_length, KEY_VALUE_HEADS, heads_per_group, HEAD_SIZE)
    key_all = low_rank_part(rotary_tables(projected_rows[:, :, heads_per_group], token_position))
    value_all = low_rank_part(projected_rows[:, :, heads_per_group + 1])

    def one_head(head_inputs):
        query_head, key_head, value_head = head_inputs
        scores = low_back(jnp.einsum('qjd,kd->jqk', query_head, key_head, precision=lax.Precision.HIGHEST)) * score_scale
        scores = jnp.where(visible[None], scores, -1e+30)
        probability = jax.nn.softmax(scores, axis=-1)
        return jnp.einsum('jqk,kd->qjd', low_rank_part(probability), value_head, precision=lax.Precision.HIGHEST)
    heads_out = lax.map(jax.checkpoint(one_head), (query_rows.transpose(1, 0, 2, 3), key_all.transpose(1, 0, 2), value_all.transpose(1, 0, 2)))
    attn = low_back(low_rank_part(heads_out.transpose(1, 0, 2, 3).reshape(token_length, QUERY_HEADS * HEAD_SIZE)))
    rank_out = low_back(low_rank_part(highest(attn, stacked(out_a).T))) * select
    residual = inputs_f + low_back(highest(attn, wo) + highest(rank_out, stacked(out_b)))
    normed_ffn = low_rank_part(normalize(residual, ffn_gain))
    rank_gate = low_back(low_rank_part(highest(normed_ffn, stacked(ffn_in_a[:, 0]).T))) * select
    rank_upper = low_back(low_rank_part(highest(normed_ffn, stacked(ffn_in_a[:, 1]).T))) * select
    gate_val = low_back(highest(normed_ffn, ffn[:, 0]) + highest(rank_gate, stacked(ffn_in_b[:, 0])))
    upper_val = low_back(highest(normed_ffn, ffn[:, 1]) + highest(rank_upper, stacked(ffn_in_b[:, 1])))
    hidden = low_rank_part(jax.nn.silu(gate_val) * upper_val)
    rank_down = low_back(low_rank_part(highest(hidden, stacked(ffn_out_a).T))) * select
    down_val = low_back(highest(hidden, ffn[:, 2].T) + highest(rank_down, stacked(ffn_out_b)))
    return residual + down_val

def reference(tokens, out_grad, block_role, adapter_of, attn_gain, ffn_gain, wqkv, wo, ffn, qkv_a, qkv_b, out_a, out_b, ffn_in_a, ffn_in_b, ffn_out_a, ffn_out_b):
    weights = (attn_gain.astype(jnp.float32), ffn_gain.astype(jnp.float32), wqkv.astype(jnp.float32), wo.astype(jnp.float32), ffn.astype(jnp.float32))
    adapters = (qkv_a.astype(jnp.float32), qkv_b.astype(jnp.float32), out_a.astype(jnp.float32), out_b.astype(jnp.float32), ffn_in_a.astype(jnp.float32), ffn_in_b.astype(jnp.float32), ffn_out_a.astype(jnp.float32), ffn_out_b.astype(jnp.float32))

    def forward(inputs_all, stacks):

        def one_group(group_inputs):
            inputs_f, role_row, owner_row = group_inputs
            return jax.checkpoint(group_forward)(inputs_f, role_row, owner_row, stacks, weights)
        return lax.map(one_group, (inputs_all, block_role, adapter_of))
    output, pullback = jax.vjp(forward, tokens.astype(jnp.float32), adapters)
    input_grad, stack_grads = pullback(out_grad.astype(jnp.float32))
    return (output.astype(jnp.bfloat16), input_grad, stack_grads[0], stack_grads[1], stack_grads[2], stack_grads[3], stack_grads[4], stack_grads[5], stack_grads[6], stack_grads[7])
```

```python
import functools
import math

import jax
import jax.numpy as jnp
from jax import lax
from jax.experimental import pallas as pl
from jax.experimental.pallas import tpu as pltpu
from jax.sharding import PartitionSpec as P

QUERY_HEADS = 16
KEY_VALUE_HEADS = 8
HEADS_PER_GROUP = QUERY_HEADS // KEY_VALUE_HEADS
HEAD_SIZE = 128
FF = 8192
R = 16
NA = 8
PBLK = 8
CONTS = 8
BLOCK = 128
SLOTS = 16
GTOK = SLOTS * BLOCK
RANKS = NA * R

eps_norm = 1e-05
rope_base = 1000000.0
score_scale = 1.0 / math.sqrt(HEAD_SIZE)
NEG = -1e30
bf16 = jnp.bfloat16
f32 = jnp.float32


def nn(a, b):
    return jnp.dot(a, b, preferred_element_type=f32)


def nt(a, b):
    return lax.dot_general(a, b, (((1,), (1,)), ((), ())), preferred_element_type=f32)


def tn(a, b):
    return lax.dot_general(a, b, (((0,), (0,)), ((), ())), preferred_element_type=f32)


def norm_forward(values, gain):
    inverse = lax.rsqrt(jnp.mean(values * values, axis=-1, keepdims=True) + eps_norm)
    return (values * inverse * gain, inverse)


def norm_backward(values, inverse, gain, grads):
    weighted = grads * gain
    return inverse * weighted - values * (inverse * inverse * inverse) * jnp.mean(
        values * weighted, axis=-1, keepdims=True
    )


def rope_tables():
    half = HEAD_SIZE // 2
    frequency = jnp.exp(
        jnp.arange(half, dtype=f32) * (-2.0 * math.log(rope_base) / HEAD_SIZE)
    )
    position = jnp.arange((PBLK + 1) * BLOCK, dtype=f32)
    angles = position[:, None] * frequency[None, :]
    cosine, sine = jnp.cos(angles), jnp.sin(angles)
    return (
        jnp.concatenate([cosine, cosine], axis=1),
        jnp.concatenate([-sine, sine], axis=1),
    )


def select_matrix(role_row, owner_row):
    matches = (role_row - PBLK)[:, None] == jnp.arange(CONTS, dtype=jnp.int32)[None, :]
    owner_slot = jnp.max(jnp.where(matches, owner_row[None, :], -1), axis=1)
    owner_tok = jnp.repeat(owner_slot, BLOCK)
    column_owner = jnp.arange(RANKS, dtype=jnp.int32) // R
    return (owner_tok[:, None] == column_owner[None, :]).astype(f32)


def half_roll(x):
    return pltpu.roll(x, shift=HEAD_SIZE // 2, axis=1)


def causal_block(heads):
    rows = lax.broadcasted_iota(jnp.int32, (heads * BLOCK, BLOCK), 0) % BLOCK
    cols = lax.broadcasted_iota(jnp.int32, (heads * BLOCK, BLOCK), 1)
    return cols <= rows


def stack_heads(x):
    heads = x.shape[1] // HEAD_SIZE
    return jnp.concatenate(
        [x[:, j * HEAD_SIZE : (j + 1) * HEAD_SIZE] for j in range(heads)], axis=0
    )


def unstack_heads(x):
    heads = x.shape[0] // BLOCK
    return jnp.concatenate([x[j * BLOCK : (j + 1) * BLOCK] for j in range(heads)], axis=1)


def slot_rows(slot_ref, role):
    return pl.ds(pl.multiple_of(slot_ref[role] * BLOCK, BLOCK), BLOCK)


def role_rows(role):
    return pl.ds(pl.multiple_of(role * BLOCK, BLOCK), BLOCK)


def stack_rows(role, heads):
    n = heads * BLOCK
    return pl.ds(pl.multiple_of(role * n, n), n)


def attention_forward_kernel(slot_ref, proj_ref, cos_ref, sin_ref, attn_ref, qs_ref, kv_ref, lse_ref):
    heads = attn_ref.shape[1] // HEAD_SIZE
    qcols = heads * HEAD_SIZE

    def prepare(role, _):
        rows = slot_rows(slot_ref, role)
        table = role_rows(jnp.minimum(role, PBLK))
        cosine, sine = cos_ref[table, :], sin_ref[table, :]

        def turned(c):
            v = proj_ref[rows, c * HEAD_SIZE : (c + 1) * HEAD_SIZE]
            return (v * cosine + half_roll(v) * sine).astype(bf16)

        qs_ref[stack_rows(role, heads), :] = jnp.concatenate(
            [turned(j) for j in range(heads)], axis=0
        )
        kv_ref[role_rows(role), :HEAD_SIZE] = turned(heads)
        kv_ref[role_rows(role), HEAD_SIZE:] = proj_ref[rows, qcols + HEAD_SIZE :].astype(bf16)
        return 0

    lax.fori_loop(0, SLOTS, prepare, 0)
    causal = causal_block(heads)

    def one(role, prompt_blocks, own):
        q = qs_ref[stack_rows(role, heads), :]
        own_k = kv_ref[own, :HEAD_SIZE]
        own_v = kv_ref[own, HEAD_SIZE:]
        s_own = jnp.where(causal, nt(q, own_k) * score_scale, NEG)
        top = jnp.max(s_own, axis=1, keepdims=True)
        if prompt_blocks:
            n = prompt_blocks * BLOCK
            s_pre = nt(q, kv_ref[:n, :HEAD_SIZE]) * score_scale
            top = jnp.maximum(top, jnp.max(s_pre, axis=1, keepdims=True))
        e_own = jnp.exp(s_own - top)
        total = jnp.sum(e_own, axis=1, keepdims=True)
        out = nn(e_own.astype(bf16), own_v)
        if prompt_blocks:
            e_pre = jnp.exp(s_pre - top)
            total = total + jnp.sum(e_pre, axis=1, keepdims=True)
            out = out + nn(e_pre.astype(bf16), kv_ref[:n, HEAD_SIZE:])
        out = out / total
        lse_ref[stack_rows(role, heads), :] = top + jnp.log(total)
        attn_ref[slot_rows(slot_ref, role), :] = unstack_heads(out).astype(bf16)

    for role in range(PBLK):
        one(role, role, slice(role * BLOCK, (role + 1) * BLOCK))

    def later(c, _):
        one(PBLK + c, PBLK, role_rows(PBLK + c))
        return 0

    lax.fori_loop(0, CONTS, later, 0)


def attention_forward(slots, projected, cosine, sine):
    tokens = projected.shape[0]
    heads = projected.shape[1] // HEAD_SIZE - 2
    vm = pl.BlockSpec(memory_space=pltpu.VMEM)
    return pl.pallas_call(
        attention_forward_kernel,
        out_shape=(
            jax.ShapeDtypeStruct((tokens, heads * HEAD_SIZE), bf16),
            jax.ShapeDtypeStruct((tokens * heads, HEAD_SIZE), bf16),
            jax.ShapeDtypeStruct((tokens, 2 * HEAD_SIZE), bf16),
            jax.ShapeDtypeStruct((tokens * heads, 1), f32),
        ),
        in_specs=[pl.BlockSpec(memory_space=pltpu.SMEM), vm, vm, vm],
        out_specs=(vm, vm, vm, vm),
        cost_estimate=pl.CostEstimate(
            flops=4 * 10**9, bytes_accessed=10 * 2**20, transcendentals=4 * 10**6
        ),
        name="attention_forward",
    )(slots, projected, cosine, sine)


def attention_backward_kernel(
    slot_ref, qs_ref, kv_ref, lse_ref, grad_ref, cos_ref, sin_ref, out_ref, dk_ref, dv_ref
):
    heads = grad_ref.shape[1] // HEAD_SIZE
    qcols = heads * HEAD_SIZE
    dk_ref[...] = jnp.zeros_like(dk_ref)
    dv_ref[...] = jnp.zeros_like(dv_ref)
    causal = causal_block(heads)

    def turned_back(g, role):
        table = role_rows(jnp.minimum(role, PBLK))
        return g * cos_ref[table, :] - half_roll(g) * sin_ref[table, :]

    def one(role, prompt_blocks, own):
        q = qs_ref[stack_rows(role, heads), :]
        lse = lse_ref[stack_rows(role, heads), :]
        rows = slot_rows(slot_ref, role)
        g = stack_heads(grad_ref[rows, :])
        own_k = kv_ref[own, :HEAD_SIZE]
        own_v = kv_ref[own, HEAD_SIZE:]
        p_own = jnp.exp(jnp.where(causal, nt(q, own_k) * score_scale, NEG) - lse)
        dp_own = nt(g, own_v)
        centre = jnp.sum(p_own * dp_own, axis=1, keepdims=True)
        if prompt_blocks:
            n = prompt_blocks * BLOCK
            pre_k = kv_ref[:n, :HEAD_SIZE]
            p_pre = jnp.exp(nt(q, pre_k) * score_scale - lse)
            dp_pre = nt(g, kv_ref[:n, HEAD_SIZE:])
            centre = centre + jnp.sum(p_pre * dp_pre, axis=1, keepdims=True)
        ds_own = (p_own * (dp_own - centre) * score_scale).astype(bf16)
        dq = nn(ds_own, own_k)
        dk_ref[own, :] += tn(ds_own, q)
        dv_ref[own, :] += tn(p_own.astype(bf16), g)
        if prompt_blocks:
            ds_pre = (p_pre * (dp_pre - centre) * score_scale).astype(bf16)
            dq = dq + nn(ds_pre, pre_k)
            dk_ref[:n, :] += tn(ds_pre, q)
            dv_ref[:n, :] += tn(p_pre.astype(bf16), g)
        for j in range(heads):
            out_ref[rows, j * HEAD_SIZE : (j + 1) * HEAD_SIZE] = turned_back(
                dq[j * BLOCK : (j + 1) * BLOCK], role
            ).astype(bf16)

    for role in range(PBLK):
        one(role, role, slice(role * BLOCK, (role + 1) * BLOCK))

    def later(c, _):
        one(PBLK + c, PBLK, role_rows(PBLK + c))
        return 0

    lax.fori_loop(0, CONTS, later, 0)

    def finish(role, _):
        rows = slot_rows(slot_ref, role)
        out_ref[rows, qcols : qcols + HEAD_SIZE] = turned_back(dk_ref[role_rows(role), :], role).astype(bf16)
        out_ref[rows, qcols + HEAD_SIZE :] = dv_ref[role_rows(role), :].astype(bf16)
        return 0

    lax.fori_loop(0, SLOTS, finish, 0)


def attention_backward(slots, qs, kv, lse, grad, cosine, sine):
    tokens = kv.shape[0]
    vm = pl.BlockSpec(memory_space=pltpu.VMEM)
    return pl.pallas_call(
        attention_backward_kernel,
        out_shape=jax.ShapeDtypeStruct((tokens, grad.shape[1] + 2 * HEAD_SIZE), bf16),
        in_specs=[pl.BlockSpec(memory_space=pltpu.SMEM)] + [vm] * 6,
        out_specs=vm,
        scratch_shapes=[
            pltpu.VMEM((tokens, HEAD_SIZE), f32),
            pltpu.VMEM((tokens, HEAD_SIZE), f32),
        ],
        cost_estimate=pl.CostEstimate(
            flops=9 * 10**9, bytes_accessed=10 * 2**20, transcendentals=4 * 10**6
        ),
        name="attention_backward",
    )(slots, qs, kv, lse, grad, cosine, sine)


def gather_tokens(x):
    return lax.all_gather(x, "seq", axis=0, tiled=True)


def scatter_tokens(x):
    return lax.psum_scatter(x, "seq", scatter_dimension=0, tiled=True)


def head_columns(w, seq):
    split = seq // KEY_VALUE_HEADS
    if split == 1:
        return w
    rows, own = w.shape[0], HEADS_PER_GROUP // split
    w = w.reshape(rows, KEY_VALUE_HEADS, HEADS_PER_GROUP + 2, HEAD_SIZE)
    q = w[:, :, :HEADS_PER_GROUP].reshape(rows, KEY_VALUE_HEADS, split, own, HEAD_SIZE)
    kv = jnp.broadcast_to(
        w[:, :, None, HEADS_PER_GROUP:], (rows, KEY_VALUE_HEADS, split, 2, HEAD_SIZE)
    )
    return jnp.concatenate([q, kv], axis=3).reshape(rows, -1)


def joined_grad(g, seq):
    split = seq // KEY_VALUE_HEADS
    if split == 1:
        return g
    own = HEADS_PER_GROUP // split
    lead = g.shape[:-1]
    g = g.reshape(*lead, KEY_VALUE_HEADS, split, own + 2, HEAD_SIZE)
    q = g[..., :own, :].reshape(*lead, KEY_VALUE_HEADS, HEADS_PER_GROUP, HEAD_SIZE)
    return jnp.concatenate([q, jnp.sum(g[..., own:, :], axis=-3)], axis=-2).reshape(*lead, -1)


def column_shard(w):
    seq = lax.axis_size("seq")
    rows, columns = w.shape
    part = lax.all_to_all(w, "seq", split_axis=1, concat_axis=0, tiled=True)
    part = part.reshape(seq, rows, columns // seq)
    return lax.all_gather(part, "ad", axis=1, tiled=True).reshape(-1, columns // seq)


def local(
    tokens,
    out_grad,
    block_role,
    adapter_of,
    attn_gain,
    ffn_gain,
    wqkv,
    wo,
    ffn,
    qkv_a,
    qkv_b,
    out_a,
    out_b,
    ffn_in_a,
    ffn_in_b,
    ffn_out_a,
    ffn_out_b,
):
    own = tokens.shape[1]
    width = tokens.shape[2]
    seq = lax.axis_size("seq")
    rank_seq = lax.axis_index("seq")
    ff_part = FF // seq
    wqkv = head_columns(wqkv, seq)
    qkv_part = wqkv.shape[1] // seq
    head_part = QUERY_HEADS * HEAD_SIZE // seq
    row_start = rank_seq * own

    def my_columns(a, part):
        return lax.dynamic_slice_in_dim(a, rank_seq * part, part, a.ndim - 1)

    def stack_ad(a):
        return lax.all_gather(a, "ad", axis=0, tiled=True)

    role_row = block_role[0]
    slots = jnp.argsort(role_row).astype(jnp.int32)
    select_all = select_matrix(role_row, adapter_of[0])
    select_all_b = select_all.astype(bf16)
    select_own = lax.dynamic_slice_in_dim(select_all, row_start, own, 0)
    select_own_b = select_own.astype(bf16)
    cosine, sine = rope_tables()

    flat = lambda a: a.reshape(-1, a.shape[-1])
    first = stack_ad(jnp.concatenate([flat(qkv_a), my_columns(head_columns(flat(qkv_b), seq), qkv_part)], axis=1))
    qkv_enter, qkv_leave = first[:, :width], first[:, width:]
    second = stack_ad(
        jnp.concatenate(
            [
                flat(out_b),
                flat(ffn_in_a[:, 0]),
                flat(ffn_in_a[:, 1]),
                flat(ffn_out_b),
                my_columns(flat(out_a), head_part),
                my_columns(flat(ffn_in_b[:, 0]), ff_part),
                my_columns(flat(ffn_in_b[:, 1]), ff_part),
                my_columns(flat(ffn_out_a), ff_part),
            ],
            axis=1,
        )
    )
    cuts = [width] * 4 + [head_part] + [ff_part] * 3
    pieces, at = [], 0
    for c in cuts:
        pieces.append(second[:, at : at + c])
        at += c
    out_leave, gate_enter, upper_enter, down_leave, out_enter, gate_leave, upper_leave, down_enter = pieces

    qkv_w = column_shard(wqkv)
    out_w = lax.all_gather(wo, "ad", axis=0, tiled=True)
    w1 = column_shard(ffn[:, 0])
    w3 = column_shard(ffn[:, 1])
    w2 = column_shard(ffn[:, 2])

    inputs_f = tokens[0].astype(f32)
    normed, inverse_attn = norm_forward(inputs_f, attn_gain)
    normed_attn = normed.astype(bf16)
    normed_attn_all = gather_tokens(normed_attn)
    rank_qkv = nt(normed_attn_all, qkv_enter).astype(bf16) * select_all_b
    projected = nn(normed_attn_all, qkv_w) + nn(rank_qkv, qkv_leave)
    attn, qs, kv, lse = attention_forward(slots, projected, cosine, sine)
    branch = scatter_tokens(
        jnp.concatenate([nn(attn, out_w), nt(attn, out_enter)], axis=1).astype(bf16)
    )
    rank_out = branch[:, width:] * select_own_b
    residual = inputs_f + branch[:, :width].astype(f32) + nn(rank_out, out_leave)
    normed_two, inverse_ffn = norm_forward(residual, ffn_gain)
    normed_ffn = normed_two.astype(bf16)
    normed_ffn_all = gather_tokens(normed_ffn)
    rank_gate = nt(normed_ffn_all, gate_enter).astype(bf16) * select_all_b
    rank_upper = nt(normed_ffn_all, upper_enter).astype(bf16) * select_all_b
    gate_val = nn(normed_ffn_all, w1) + nn(rank_gate, gate_leave)
    upper_val = nn(normed_ffn_all, w3) + nn(rank_upper, upper_leave)
    sigma = jax.nn.sigmoid(gate_val)
    silu_gate = gate_val * sigma
    hidden = (silu_gate * upper_val).astype(bf16)
    down = scatter_tokens(
        jnp.concatenate([nt(hidden, w2), nt(hidden, down_enter)], axis=1).astype(bf16)
    )
    rank_down = down[:, width:] * select_own_b
    output = (
        residual + down[:, :width].astype(f32) + nn(rank_down, down_leave)
    ).astype(bf16)[None]

    grad_down = out_grad[0]
    grad_all = gather_tokens(grad_down)
    d_rank_down = (nt(grad_all, down_leave) * select_all).astype(bf16)
    d_hidden = nn(grad_all, w2) + nn(d_rank_down, down_enter)
    d_gate = (d_hidden * upper_val * sigma * (1.0 + gate_val * (1.0 - sigma))).astype(bf16)
    d_upper = (d_hidden * silu_gate).astype(bf16)
    back = scatter_tokens(
        jnp.concatenate(
            [
                nt(d_gate, w1) + nt(d_upper, w3),
                nt(d_gate, gate_leave),
                nt(d_upper, upper_leave),
            ],
            axis=1,
        ).astype(bf16)
    )
    d_rank_gate = back[:, width : width + RANKS] * select_own_b
    d_rank_upper = back[:, width + RANKS :] * select_own_b
    d_normed_ffn = (
        back[:, :width].astype(f32) + nn(d_rank_gate, gate_enter) + nn(d_rank_upper, upper_enter)
    )
    d_residual = grad_down.astype(f32) + norm_backward(
        residual, inverse_ffn, ffn_gain, d_normed_ffn
    )
    d_branch = d_residual.astype(bf16)
    d_branch_all = gather_tokens(d_branch)
    d_rank_out = (nt(d_branch_all, out_leave) * select_all).astype(bf16)
    d_attn = (nt(d_branch_all, out_w) + nn(d_rank_out, out_enter)).astype(bf16)
    d_projected = attention_backward(slots, qs, kv, lse, d_attn, cosine, sine)
    back_attn = scatter_tokens(
        jnp.concatenate([nt(d_projected, qkv_w), nt(d_projected, qkv_leave)], axis=1).astype(bf16)
    )
    d_rank_qkv = back_attn[:, width:] * select_own_b
    d_normed_attn = back_attn[:, :width].astype(f32) + nn(d_rank_qkv, qkv_enter)
    input_grad = (d_residual + norm_backward(inputs_f, inverse_attn, attn_gain, d_normed_attn))[
        None
    ]

    def reduced(partial, whole):
        cols = []
        if partial:
            part = width // seq
            stack = jnp.concatenate(
                [p.astype(bf16).reshape(RANKS, seq, part) for p in partial], axis=2
            ).transpose(1, 0, 2)
            cols.append(lax.psum_scatter(stack, "seq", scatter_dimension=0, tiled=True)[0])
        cols += [w.astype(bf16) for w in whole]
        both = jnp.concatenate(cols, axis=1)
        mine = lax.psum_scatter(both, "ad", scatter_dimension=0, tiled=True)
        return lax.all_gather(mine, "seq", axis=0)

    def unpack(arr, counts):
        out, at = [], 0
        for c in counts:
            piece = arr[:, :, at : at + c].transpose(1, 0, 2).astype(f32)
            out.append(piece.reshape(piece.shape[0] // R, R, seq * c))
            at += c
        return out

    wpart = width // seq
    early = reduced(
        [
            tn(rank_out, d_branch),
            tn(d_rank_gate, normed_ffn),
            tn(d_rank_upper, normed_ffn),
            tn(rank_down, grad_down),
        ],
        [
            tn(d_rank_out, attn),
            tn(rank_gate, d_gate),
            tn(rank_upper, d_upper),
            tn(d_rank_down, hidden),
        ],
    )
    g_out_b, g_ia0, g_ia1, g_ob, g_out_a, g_ib0, g_ib1, g_oa = unpack(
        early, [wpart] * 4 + [head_part] + [ff_part] * 3
    )
    late = reduced([tn(d_rank_qkv, normed_attn)], [tn(rank_qkv, d_projected)])
    g_qkv_a, g_qkv_b = unpack(late, [wpart, qkv_part])
    return (
        output,
        input_grad,
        g_qkv_a,
        joined_grad(g_qkv_b, seq),
        g_out_a,
        g_out_b,
        jnp.stack([g_ia0, g_ia1], axis=1),
        jnp.stack([g_ib0, g_ib1], axis=1),
        g_oa,
        g_ob,
    )


def solution(mesh):
    ad3 = P("ad", None, None)
    ad4 = P("ad", None, None, None)
    return jax.shard_map(
        local,
        mesh=mesh,
        in_specs=(
            P("ad", "seq", None),
            P("ad", "seq", None),
            P("ad", None),
            P("ad", None),
            P(),
            P(),
            P(("seq", "ad"), None),
            P(("seq", "ad"), None),
            P(("seq", "ad"), None, None),
            ad3,
            ad3,
            ad3,
            ad3,
            ad4,
            ad4,
            ad3,
            ad3,
        ),
        out_specs=(
            P("ad", "seq", None),
            P("ad", "seq", None),
            ad3,
            ad3,
            ad3,
            ad3,
            ad4,
            ad4,
            ad3,
            ad3,
        ),
        check_vma=False,
    )
```

```python
import functools
import math

import jax
import jax.numpy as jnp
from jax import lax
from jax.experimental import pallas as pl
from jax.experimental.pallas import tpu as pltpu
from jax.sharding import PartitionSpec as P

QUERY_HEADS = 16
KEY_VALUE_HEADS = 8
HEADS_PER_GROUP = QUERY_HEADS // KEY_VALUE_HEADS
HEAD_SIZE = 128
FF = 8192
R = 16
NA = 8
PBLK = 8
CONTS = 8
BLOCK = 128
SLOTS = 16
GTOK = SLOTS * BLOCK
RANKS = NA * R

eps_norm = 1e-05
rope_base = 1000000.0
score_scale = 1.0 / math.sqrt(HEAD_SIZE)
NEG = -1e30
bf16 = jnp.bfloat16
f32 = jnp.float32


def nn(a, b):
    return jnp.dot(a, b, preferred_element_type=f32)


def nt(a, b):
    return lax.dot_general(a, b, (((1,), (1,)), ((), ())), preferred_element_type=f32)


def tn(a, b):
    return lax.dot_general(a, b, (((0,), (0,)), ((), ())), preferred_element_type=f32)


def norm_forward(values, gain):
    inverse = lax.rsqrt(jnp.mean(values * values, axis=-1, keepdims=True) + eps_norm)
    return (values * inverse * gain, inverse)


def norm_backward(values, inverse, gain, grads):
    weighted = grads * gain
    return inverse * weighted - values * (inverse * inverse * inverse) * jnp.mean(
        values * weighted, axis=-1, keepdims=True
    )


def rope_tables():
    half = HEAD_SIZE // 2
    frequency = jnp.exp(
        jnp.arange(half, dtype=f32) * (-2.0 * math.log(rope_base) / HEAD_SIZE)
    )
    position = jnp.arange((PBLK + 1) * BLOCK, dtype=f32)
    angles = position[:, None] * frequency[None, :]
    cosine, sine = jnp.cos(angles), jnp.sin(angles)
    return (
        jnp.concatenate([cosine, cosine], axis=1),
        jnp.concatenate([-sine, sine], axis=1),
    )


def select_matrix(role_row, owner_row):
    matches = (role_row - PBLK)[:, None] == jnp.arange(CONTS, dtype=jnp.int32)[None, :]
    owner_slot = jnp.max(jnp.where(matches, owner_row[None, :], -1), axis=1)
    owner_tok = jnp.repeat(owner_slot, BLOCK)
    column_owner = jnp.arange(RANKS, dtype=jnp.int32) // R
    return (owner_tok[:, None] == column_owner[None, :]).astype(f32)


def half_roll(x):
    return pltpu.roll(x, shift=HEAD_SIZE // 2, axis=1)


def causal_block(heads):
    rows = lax.broadcasted_iota(jnp.int32, (heads * BLOCK, BLOCK), 0) % BLOCK
    cols = lax.broadcasted_iota(jnp.int32, (heads * BLOCK, BLOCK), 1)
    return cols <= rows


def stack_heads(x):
    heads = x.shape[1] // HEAD_SIZE
    return jnp.concatenate(
        [x[:, j * HEAD_SIZE : (j + 1) * HEAD_SIZE] for j in range(heads)], axis=0
    )


def unstack_heads(x):
    heads = x.shape[0] // BLOCK
    return jnp.concatenate([x[j * BLOCK : (j + 1) * BLOCK] for j in range(heads)], axis=1)


def slot_rows(slot_ref, role):
    return pl.ds(pl.multiple_of(slot_ref[role] * BLOCK, BLOCK), BLOCK)


def role_rows(role):
    return pl.ds(pl.multiple_of(role * BLOCK, BLOCK), BLOCK)


def stack_rows(role, heads):
    n = heads * BLOCK
    return pl.ds(pl.multiple_of(role * n, n), n)


def attention_forward_kernel(slot_ref, proj_ref, cos_ref, sin_ref, attn_ref, qs_ref, kv_ref, lse_ref):
    heads = attn_ref.shape[1] // HEAD_SIZE
    qcols = heads * HEAD_SIZE

    def prepare(role, _):
        rows = slot_rows(slot_ref, role)
        table = role_rows(jnp.minimum(role, PBLK))
        cosine, sine = cos_ref[table, :], sin_ref[table, :]

        def turned(c):
            v = proj_ref[rows, c * HEAD_SIZE : (c + 1) * HEAD_SIZE]
            return (v * cosine + half_roll(v) * sine).astype(bf16)

        qs_ref[stack_rows(role, heads), :] = jnp.concatenate(
            [turned(j) for j in range(heads)], axis=0
        )
        kv_ref[role_rows(role), :HEAD_SIZE] = turned(heads)
        kv_ref[role_rows(role), HEAD_SIZE:] = proj_ref[rows, qcols + HEAD_SIZE :].astype(bf16)
        return 0

    lax.fori_loop(0, SLOTS, prepare, 0)
    causal = causal_block(heads)

    def one(role, prompt_blocks, own):
        q = qs_ref[stack_rows(role, heads), :]
        own_k = kv_ref[own, :HEAD_SIZE]
        own_v = kv_ref[own, HEAD_SIZE:]
        s_own = jnp.where(causal, nt(q, own_k) * score_scale, NEG)
        top = jnp.max(s_own, axis=1, keepdims=True)
        if prompt_blocks:
            n = prompt_blocks * BLOCK
            s_pre = nt(q, kv_ref[:n, :HEAD_SIZE]) * score_scale
            top = jnp.maximum(top, jnp.max(s_pre, axis=1, keepdims=True))
        e_own = jnp.exp(s_own - top)
        total = jnp.sum(e_own, axis=1, keepdims=True)
        out = nn(e_own.astype(bf16), own_v)
        if prompt_blocks:
            e_pre = jnp.exp(s_pre - top)
            total = total + jnp.sum(e_pre, axis=1, keepdims=True)
            out = out + nn(e_pre.astype(bf16), kv_ref[:n, HEAD_SIZE:])
        out = out / total
        lse_ref[stack_rows(role, heads), :] = top + jnp.log(total)
        attn_ref[slot_rows(slot_ref, role), :] = unstack_heads(out).astype(bf16)

    for role in range(PBLK):
        one(role, role, slice(role * BLOCK, (role + 1) * BLOCK))

    def later(c, _):
        one(PBLK + c, PBLK, role_rows(PBLK + c))
        return 0

    lax.fori_loop(0, CONTS, later, 0)


def attention_forward(slots, projected, cosine, sine):
    tokens = projected.shape[0]
    heads = projected.shape[1] // HEAD_SIZE - 2
    vm = pl.BlockSpec(memory_space=pltpu.VMEM)
    return pl.pallas_call(
        attention_forward_kernel,
        out_shape=(
            jax.ShapeDtypeStruct((tokens, heads * HEAD_SIZE), bf16),
            jax.ShapeDtypeStruct((tokens * heads, HEAD_SIZE), bf16),
            jax.ShapeDtypeStruct((tokens, 2 * HEAD_SIZE), bf16),
            jax.ShapeDtypeStruct((tokens * heads, 1), f32),
        ),
        in_specs=[pl.BlockSpec(memory_space=pltpu.SMEM), vm, vm, vm],
        out_specs=(vm, vm, vm, vm),
        cost_estimate=pl.CostEstimate(
            flops=4 * 10**9, bytes_accessed=10 * 2**20, transcendentals=4 * 10**6
        ),
        name="attention_forward",
    )(slots, projected, cosine, sine)


def attention_backward_kernel(
    slot_ref, qs_ref, kv_ref, lse_ref, grad_ref, cos_ref, sin_ref, out_ref, dk_ref, dv_ref
):
    heads = grad_ref.shape[1] // HEAD_SIZE
    qcols = heads * HEAD_SIZE
    dk_ref[...] = jnp.zeros_like(dk_ref)
    dv_ref[...] = jnp.zeros_like(dv_ref)
    causal = causal_block(heads)

    def turned_back(g, role):
        table = role_rows(jnp.minimum(role, PBLK))
        return g * cos_ref[table, :] - half_roll(g) * sin_ref[table, :]

    def one(role, prompt_blocks, own):
        q = qs_ref[stack_rows(role, heads), :]
        lse = lse_ref[stack_rows(role, heads), :]
        rows = slot_rows(slot_ref, role)
        g = stack_heads(grad_ref[rows, :])
        own_k = kv_ref[own, :HEAD_SIZE]
        own_v = kv_ref[own, HEAD_SIZE:]
        p_own = jnp.exp(jnp.where(causal, nt(q, own_k) * score_scale, NEG) - lse)
        dp_own = nt(g, own_v)
        centre = jnp.sum(p_own * dp_own, axis=1, keepdims=True)
        if prompt_blocks:
            n = prompt_blocks * BLOCK
            pre_k = kv_ref[:n, :HEAD_SIZE]
            p_pre = jnp.exp(nt(q, pre_k) * score_scale - lse)
            dp_pre = nt(g, kv_ref[:n, HEAD_SIZE:])
            centre = centre + jnp.sum(p_pre * dp_pre, axis=1, keepdims=True)
        ds_own = (p_own * (dp_own - centre) * score_scale).astype(bf16)
        dq = nn(ds_own, own_k)
        dk_ref[own, :] += tn(ds_own, q)
        dv_ref[own, :] += tn(p_own.astype(bf16), g)
        if prompt_blocks:
            ds_pre = (p_pre * (dp_pre - centre) * score_scale).astype(bf16)
            dq = dq + nn(ds_pre, pre_k)
            dk_ref[:n, :] += tn(ds_pre, q)
            dv_ref[:n, :] += tn(p_pre.astype(bf16), g)
        for j in range(heads):
            out_ref[rows, j * HEAD_SIZE : (j + 1) * HEAD_SIZE] = turned_back(
                dq[j * BLOCK : (j + 1) * BLOCK], role
            ).astype(bf16)

    for role in range(PBLK):
        one(role, role, slice(role * BLOCK, (role + 1) * BLOCK))

    def later(c, _):
        one(PBLK + c, PBLK, role_rows(PBLK + c))
        return 0

    lax.fori_loop(0, CONTS, later, 0)

    def finish(role, _):
        rows = slot_rows(slot_ref, role)
        out_ref[rows, qcols : qcols + HEAD_SIZE] = turned_back(dk_ref[role_rows(role), :], role).astype(bf16)
        out_ref[rows, qcols + HEAD_SIZE :] = dv_ref[role_rows(role), :].astype(bf16)
        return 0

    lax.fori_loop(0, SLOTS, finish, 0)


def attention_backward(slots, qs, kv, lse, grad, cosine, sine):
    tokens = kv.shape[0]
    vm = pl.BlockSpec(memory_space=pltpu.VMEM)
    return pl.pallas_call(
        attention_backward_kernel,
        out_shape=jax.ShapeDtypeStruct((tokens, grad.shape[1] + 2 * HEAD_SIZE), bf16),
        in_specs=[pl.BlockSpec(memory_space=pltpu.SMEM)] + [vm] * 6,
        out_specs=vm,
        scratch_shapes=[
            pltpu.VMEM((tokens, HEAD_SIZE), f32),
            pltpu.VMEM((tokens, HEAD_SIZE), f32),
        ],
        cost_estimate=pl.CostEstimate(
            flops=9 * 10**9, bytes_accessed=10 * 2**20, transcendentals=4 * 10**6
        ),
        name="attention_backward",
    )(slots, qs, kv, lse, grad, cosine, sine)


PLANE = 8


def neighbours():
    me = lax.axis_index("seq")
    core, x, y = me % 2, (me // 2) % 2, me // 4
    p = me + 1 - 2 * core
    nx = me + 2 - 4 * x
    ny = me + 4 - 8 * y
    nd = nx + 4 - 8 * y
    return me, p, nx, ny, nd


def across(i):
    return i + 1 - 2 * (i % 2)


def greet(*others):
    barrier = pltpu.get_barrier_semaphore()
    for other in others:
        pl.semaphore_signal(
            barrier, inc=1, device_id={"seq": other}, device_id_type=pl.DeviceIdType.MESH
        )
    pl.semaphore_wait(barrier, len(others))


class Links:
    def __init__(self, send_sem, recv_sem):
        self.send_sem, self.recv_sem, self.made = send_sem, recv_sem, {}

    def start(self, k, src, dst, to):
        copy = pltpu.make_async_remote_copy(
            src_ref=src,
            dst_ref=dst,
            send_sem=self.send_sem.at[k],
            recv_sem=self.recv_sem.at[k],
            device_id={"seq": to},
            device_id_type=pl.DeviceIdType.MESH,
        )
        copy.start()
        self.made[k] = copy

    def arrived(self, k):
        self.made[k].wait_recv()

    def drain(self):
        for copy in self.made.values():
            copy.wait_send()


def gather_kernel(own_ref, all_ref, send_sem, recv_sem):
    own = own_ref.shape[0]
    half = own // 2
    me, p, nx, ny, nd = neighbours()
    greet(p, nx, ny)
    links = Links(send_sem, recv_sem)

    def piece(i, h):
        return all_ref.at[pl.ds(pl.multiple_of(i * own + h * half, half), half), :]

    mine = own_ref.at
    links.start(0, mine[:half, :], piece(me, 0), nx)
    links.start(1, mine[half:, :], piece(me, 1), ny)
    links.start(2, mine[half:, :], piece(me, 1), nx)
    links.start(3, mine[:half, :], piece(me, 0), ny)
    block = all_ref.at[pl.ds(pl.multiple_of(me * own, own), own), :]
    links.start(4, own_ref, block, p)
    all_ref[pl.ds(pl.multiple_of(me * own, own), own), :] = own_ref[...]

    links.arrived(0)
    links.start(5, piece(nx, 0), piece(nx, 0), ny)
    links.start(7, piece(nx, 0), piece(nx, 0), p)
    links.arrived(1)
    links.start(6, piece(ny, 1), piece(ny, 1), nx)
    links.start(8, piece(ny, 1), piece(ny, 1), p)
    links.arrived(2)
    links.start(9, piece(nx, 1), piece(nx, 1), p)
    links.arrived(3)
    links.start(10, piece(ny, 0), piece(ny, 0), p)
    links.arrived(5)
    links.start(11, piece(nd, 0), piece(nd, 0), p)
    links.arrived(6)
    links.start(12, piece(nd, 1), piece(nd, 1), p)
    for k in (4, 7, 8, 9, 10, 11, 12):
        links.arrived(k)
    links.drain()


def gather_tokens(x):
    if lax.axis_size("seq") != PLANE:
        return lax.all_gather(x, "seq", axis=0, tiled=True)
    own, width = x.shape
    vm = pl.BlockSpec(memory_space=pltpu.VMEM)
    return pl.pallas_call(
        gather_kernel,
        out_shape=jax.ShapeDtypeStruct((PLANE * own, width), x.dtype),
        in_specs=[vm],
        out_specs=vm,
        scratch_shapes=[pltpu.SemaphoreType.DMA((13,)), pltpu.SemaphoreType.DMA((13,))],
        compiler_params=pltpu.CompilerParams(collective_id=1, has_side_effects=True),
        cost_estimate=pl.CostEstimate(
            flops=0, bytes_accessed=10 * PLANE * own * width, transcendentals=0
        ),
        name="gather_tokens",
    )(x)


COLS = 256


def scatter_kernel(modes, *refs):
    n = len(modes)
    a_refs, b_refs, r_refs = refs[:n], refs[n : 2 * n], refs[2 * n : 3 * n]
    out_ref, rank_ref, theirs, cores, sums, relay, last, send_sem, recv_sem = refs[3 * n :]
    own, width = out_ref.shape
    ranks = rank_ref.shape[1]
    half = own // 2
    per = ranks // n
    me, p, nx, ny, nd = neighbours()
    greet(p, nx, ny)
    links = Links(send_sem, recv_sem)

    def product(i, store):
        rows = pl.ds(pl.multiple_of(i * own, own), own)

        def tile(t, _):
            cols = pl.ds(pl.multiple_of(t * COLS, COLS), COLS)
            total = None
            for a, b, transposed in zip(a_refs, b_refs, modes):
                term = nt(a[rows, :], b[cols, :]) if transposed else nn(a[rows, :], b[:, cols])
                total = term if total is None else total + term
            store(cols, total)
            return 0

        lax.fori_loop(0, width // COLS, tile, 0)
        for j, (a, r) in enumerate(zip(a_refs, r_refs)):
            store(slice(width + j * per, width + (j + 1) * per), nt(a[rows, :], r[...]))

    def for_partner(slot, i):
        def store(cols, value):
            theirs[slot, :, cols] = value.astype(bf16)

        product(across(i), store)
        links.start(slot, theirs.at[slot], cores.at[slot], p)

    def chip_sum(slot, i):
        def store(cols, value):
            sums[slot, :, cols] = (value + cores[slot, :, cols].astype(f32)).astype(bf16)

        product(i, store)

    for_partner(0, nd)
    for_partner(1, nx)
    links.arrived(0)
    chip_sum(0, nd)
    links.start(4, sums.at[0, :half], relay.at[0], nx)
    links.start(5, sums.at[0, half:], relay.at[1], ny)
    links.arrived(1)
    chip_sum(1, nx)
    links.start(6, sums.at[1, :half], last.at[0, :half], nx)
    for_partner(2, ny)
    for_partner(3, me)
    links.arrived(2)
    chip_sum(2, ny)
    links.start(7, sums.at[2, half:], last.at[1, half:], ny)
    links.arrived(5)
    sums[1, half:, :] = (sums[1, half:, :].astype(f32) + relay[1].astype(f32)).astype(bf16)
    links.start(8, sums.at[1, half:], last.at[0, half:], nx)
    links.arrived(4)
    sums[2, :half, :] = (sums[2, :half, :].astype(f32) + relay[0].astype(f32)).astype(bf16)
    links.start(9, sums.at[2, :half], last.at[1, :half], ny)
    links.arrived(3)

    def keep(cols, value):
        value = value + cores[3, :, cols].astype(f32)
        if isinstance(cols, slice):
            rank_ref[:, cols.start - width : cols.stop - width] = value
        else:
            out_ref[:, cols] = value

    product(me, keep)
    for k in (6, 7, 8, 9):
        links.arrived(k)
    both = lambda cols: last[0, :, cols].astype(f32) + last[1, :, cols].astype(f32)
    out_ref[...] = out_ref[...] + both(slice(0, width))
    rank_ref[...] = rank_ref[...] + both(slice(width, width + ranks))
    links.drain()


def scatter_products(terms, collective_id):
    modes = tuple(t[3] for t in terms)
    a, b, r = ([t[k] for t in terms] for k in range(3))
    width = b[0].shape[0] if modes[0] else b[0].shape[1]
    ranks = sum(x.shape[0] for x in r)
    seq = lax.axis_size("seq")
    rows = a[0].shape[0]
    own = rows // seq
    if seq != PLANE:
        total = sum(nt(x, y) if m else nn(x, y) for x, y, m in zip(a, b, modes))
        both = jnp.concatenate([total] + [nt(x, y) for x, y in zip(a, r)], axis=1).astype(bf16)
        both = lax.psum_scatter(both, "seq", scatter_dimension=0, tiled=True).astype(f32)
        return both[:, :width], both[:, width:]
    vm = pl.BlockSpec(memory_space=pltpu.VMEM)
    whole = width + ranks
    depth = sum(x.shape[1] for x in a)
    return pl.pallas_call(
        functools.partial(scatter_kernel, modes),
        out_shape=(
            jax.ShapeDtypeStruct((own, width), f32),
            jax.ShapeDtypeStruct((own, ranks), f32),
        ),
        in_specs=[vm] * (3 * len(terms)),
        out_specs=(vm, vm),
        scratch_shapes=[
            pltpu.VMEM((4, own, whole), bf16),
            pltpu.VMEM((4, own, whole), bf16),
            pltpu.VMEM((3, own, whole), bf16),
            pltpu.VMEM((2, own // 2, whole), bf16),
            pltpu.VMEM((2, own, whole), bf16),
            pltpu.SemaphoreType.DMA((10,)),
            pltpu.SemaphoreType.DMA((10,)),
        ],
        compiler_params=pltpu.CompilerParams(collective_id=collective_id, has_side_effects=True),
        cost_estimate=pl.CostEstimate(
            flops=2 * rows * depth * whole + 4 * 10**10,
            bytes_accessed=rows * depth * 4,
            transcendentals=0,
        ),
        name=f"scatter_products_{collective_id}",
    )(*a, *b, *r)


def head_columns(w, seq):
    split = seq // KEY_VALUE_HEADS
    if split == 1:
        return w
    rows, own = w.shape[0], HEADS_PER_GROUP // split
    w = w.reshape(rows, KEY_VALUE_HEADS, HEADS_PER_GROUP + 2, HEAD_SIZE)
    q = w[:, :, :HEADS_PER_GROUP].reshape(rows, KEY_VALUE_HEADS, split, own, HEAD_SIZE)
    kv = jnp.broadcast_to(
        w[:, :, None, HEADS_PER_GROUP:], (rows, KEY_VALUE_HEADS, split, 2, HEAD_SIZE)
    )
    return jnp.concatenate([q, kv], axis=3).reshape(rows, -1)


def joined_grad(g, seq):
    split = seq // KEY_VALUE_HEADS
    if split == 1:
        return g
    own = HEADS_PER_GROUP // split
    lead = g.shape[:-1]
    g = g.reshape(*lead, KEY_VALUE_HEADS, split, own + 2, HEAD_SIZE)
    q = g[..., :own, :].reshape(*lead, KEY_VALUE_HEADS, HEADS_PER_GROUP, HEAD_SIZE)
    return jnp.concatenate([q, jnp.sum(g[..., own:, :], axis=-3)], axis=-2).reshape(*lead, -1)


def column_shard(w):
    seq = lax.axis_size("seq")
    rows, columns = w.shape
    part = lax.all_to_all(w, "seq", split_axis=1, concat_axis=0, tiled=True)
    part = part.reshape(seq, rows, columns // seq)
    return lax.all_gather(part, "ad", axis=1, tiled=True).reshape(-1, columns // seq)


def local(
    tokens,
    out_grad,
    block_role,
    adapter_of,
    attn_gain,
    ffn_gain,
    wqkv,
    wo,
    ffn,
    qkv_a,
    qkv_b,
    out_a,
    out_b,
    ffn_in_a,
    ffn_in_b,
    ffn_out_a,
    ffn_out_b,
):
    own = tokens.shape[1]
    width = tokens.shape[2]
    seq = lax.axis_size("seq")
    rank_seq = lax.axis_index("seq")
    ff_part = FF // seq
    wqkv = head_columns(wqkv, seq)
    qkv_part = wqkv.shape[1] // seq
    head_part = QUERY_HEADS * HEAD_SIZE // seq
    row_start = rank_seq * own

    def my_columns(a, part):
        return lax.dynamic_slice_in_dim(a, rank_seq * part, part, a.ndim - 1)

    def stack_ad(a):
        return lax.all_gather(a, "ad", axis=0, tiled=True)

    role_row = block_role[0]
    slots = jnp.argsort(role_row).astype(jnp.int32)
    select_all = select_matrix(role_row, adapter_of[0])
    select_all_b = select_all.astype(bf16)
    select_own = lax.dynamic_slice_in_dim(select_all, row_start, own, 0)
    select_own_b = select_own.astype(bf16)
    cosine, sine = rope_tables()

    flat = lambda a: a.reshape(-1, a.shape[-1])
    first = stack_ad(jnp.concatenate([flat(qkv_a), my_columns(head_columns(flat(qkv_b), seq), qkv_part)], axis=1))
    qkv_enter, qkv_leave = first[:, :width], first[:, width:]
    second = stack_ad(
        jnp.concatenate(
            [
                flat(out_b),
                flat(ffn_in_a[:, 0]),
                flat(ffn_in_a[:, 1]),
                flat(ffn_out_b),
                my_columns(flat(out_a), head_part),
                my_columns(flat(ffn_in_b[:, 0]), ff_part),
                my_columns(flat(ffn_in_b[:, 1]), ff_part),
                my_columns(flat(ffn_out_a), ff_part),
            ],
            axis=1,
        )
    )
    cuts = [width] * 4 + [head_part] + [ff_part] * 3
    pieces, at = [], 0
    for c in cuts:
        pieces.append(second[:, at : at + c])
        at += c
    out_leave, gate_enter, upper_enter, down_leave, out_enter, gate_leave, upper_leave, down_enter = pieces

    qkv_w = column_shard(wqkv)
    out_w = lax.all_gather(wo, "ad", axis=0, tiled=True)
    w1 = column_shard(ffn[:, 0])
    w3 = column_shard(ffn[:, 1])
    w2 = column_shard(ffn[:, 2])

    inputs_f = tokens[0].astype(f32)
    normed, inverse_attn = norm_forward(inputs_f, attn_gain)
    normed_attn = normed.astype(bf16)
    normed_attn_all = gather_tokens(normed_attn)
    rank_qkv = nt(normed_attn_all, qkv_enter).astype(bf16) * select_all_b
    projected = nn(normed_attn_all, qkv_w) + nn(rank_qkv, qkv_leave)
    attn, qs, kv, lse = attention_forward(slots, projected, cosine, sine)
    branch, rank_out = scatter_products([(attn, out_w, out_enter, False)], 2)
    rank_out = rank_out.astype(bf16) * select_own_b
    residual = inputs_f + branch + nn(rank_out, out_leave)
    normed_two, inverse_ffn = norm_forward(residual, ffn_gain)
    normed_ffn = normed_two.astype(bf16)
    normed_ffn_all = gather_tokens(normed_ffn)
    rank_gate = nt(normed_ffn_all, gate_enter).astype(bf16) * select_all_b
    rank_upper = nt(normed_ffn_all, upper_enter).astype(bf16) * select_all_b
    gate_val = nn(normed_ffn_all, w1) + nn(rank_gate, gate_leave)
    upper_val = nn(normed_ffn_all, w3) + nn(rank_upper, upper_leave)
    sigma = jax.nn.sigmoid(gate_val)
    silu_gate = gate_val * sigma
    hidden = (silu_gate * upper_val).astype(bf16)
    down, rank_down = scatter_products([(hidden, w2, down_enter, True)], 3)
    rank_down = rank_down.astype(bf16) * select_own_b
    output = (residual + down + nn(rank_down, down_leave)).astype(bf16)[None]

    grad_down = out_grad[0]
    grad_all = gather_tokens(grad_down)
    d_rank_down = (nt(grad_all, down_leave) * select_all).astype(bf16)
    d_hidden = nn(grad_all, w2) + nn(d_rank_down, down_enter)
    d_gate = (d_hidden * upper_val * sigma * (1.0 + gate_val * (1.0 - sigma))).astype(bf16)
    d_upper = (d_hidden * silu_gate).astype(bf16)
    back, back_rank = scatter_products(
        [(d_gate, w1, gate_leave, True), (d_upper, w3, upper_leave, True)], 4
    )
    d_rank_gate = (back_rank[:, :RANKS] * select_own).astype(bf16)
    d_rank_upper = (back_rank[:, RANKS:] * select_own).astype(bf16)
    d_normed_ffn = back + nn(d_rank_gate, gate_enter) + nn(d_rank_upper, upper_enter)
    d_residual = grad_down.astype(f32) + norm_backward(
        residual, inverse_ffn, ffn_gain, d_normed_ffn
    )
    d_branch = d_residual.astype(bf16)
    d_branch_all = gather_tokens(d_branch)
    d_rank_out = (nt(d_branch_all, out_leave) * select_all).astype(bf16)
    d_attn = (nt(d_branch_all, out_w) + nn(d_rank_out, out_enter)).astype(bf16)
    d_projected = attention_backward(slots, qs, kv, lse, d_attn, cosine, sine)
    back_attn, back_rank_qkv = scatter_products([(d_projected, qkv_w, qkv_leave, True)], 5)
    d_rank_qkv = (back_rank_qkv * select_own).astype(bf16)
    d_normed_attn = back_attn + nn(d_rank_qkv, qkv_enter)
    input_grad = (d_residual + norm_backward(inputs_f, inverse_attn, attn_gain, d_normed_attn))[
        None
    ]

    def reduced(partial, whole):
        cols = []
        if partial:
            part = width // seq
            stack = jnp.concatenate(
                [p.astype(bf16).reshape(RANKS, seq, part) for p in partial], axis=2
            ).transpose(1, 0, 2)
            cols.append(lax.psum_scatter(stack, "seq", scatter_dimension=0, tiled=True)[0])
        cols += [w.astype(bf16) for w in whole]
        both = jnp.concatenate(cols, axis=1)
        mine = lax.psum_scatter(both, "ad", scatter_dimension=0, tiled=True)
        return lax.all_gather(mine, "seq", axis=0)

    def unpack(arr, counts):
        out, at = [], 0
        for c in counts:
            piece = arr[:, :, at : at + c].transpose(1, 0, 2).astype(f32)
            out.append(piece.reshape(piece.shape[0] // R, R, seq * c))
            at += c
        return out

    wpart = width // seq
    early = reduced(
        [
            tn(rank_out, d_branch),
            tn(d_rank_gate, normed_ffn),
            tn(d_rank_upper, normed_ffn),
            tn(rank_down, grad_down),
        ],
        [
            tn(d_rank_out, attn),
            tn(rank_gate, d_gate),
            tn(rank_upper, d_upper),
            tn(d_rank_down, hidden),
        ],
    )
    g_out_b, g_ia0, g_ia1, g_ob, g_out_a, g_ib0, g_ib1, g_oa = unpack(
        early, [wpart] * 4 + [head_part] + [ff_part] * 3
    )
    late = reduced([tn(d_rank_qkv, normed_attn)], [tn(rank_qkv, d_projected)])
    g_qkv_a, g_qkv_b = unpack(late, [wpart, qkv_part])
    return (
        output,
        input_grad,
        g_qkv_a,
        joined_grad(g_qkv_b, seq),
        g_out_a,
        g_out_b,
        jnp.stack([g_ia0, g_ia1], axis=1),
        jnp.stack([g_ib0, g_ib1], axis=1),
        g_oa,
        g_ob,
    )


def solution(mesh):
    ad3 = P("ad", None, None)
    ad4 = P("ad", None, None, None)
    return jax.shard_map(
        local,
        mesh=mesh,
        in_specs=(
            P("ad", "seq", None),
            P("ad", "seq", None),
            P("ad", None),
            P("ad", None),
            P(),
            P(),
            P(("seq", "ad"), None),
            P(("seq", "ad"), None),
            P(("seq", "ad"), None, None),
            ad3,
            ad3,
            ad3,
            ad3,
            ad4,
            ad4,
            ad3,
            ad3,
        ),
        out_specs=(
            P("ad", "seq", None),
            P("ad", "seq", None),
            ad3,
            ad3,
            ad3,
            ad3,
            ad4,
            ad4,
            ad3,
            ad3,
        ),
        check_vma=False,
    )
```

```python
import functools
import math

import jax
import jax.numpy as jnp
from jax import lax
from jax.experimental import pallas as pl
from jax.experimental.pallas import tpu as pltpu
from jax.sharding import PartitionSpec as P


QUERY_HEADS = 16
KEY_VALUE_HEADS = 8
HEADS_PER_GROUP = QUERY_HEADS // KEY_VALUE_HEADS
HEAD_SIZE = 128
FF = 8192
R = 16
NA = 8
PBLK = 8
CONTS = 8
BLOCK = 128
SLOTS = 16
RANKS = NA * R

eps_norm = 1e-05
rope_base = 1000000.0
score_scale = 1.0 / math.sqrt(HEAD_SIZE)
NEG = -1e30
bf16 = jnp.bfloat16
f32 = jnp.float32


def nn(a, b):
    return jnp.dot(a, b, preferred_element_type=f32)


def nt(a, b):
    return lax.dot_general(a, b, (((1,), (1,)), ((), ())), preferred_element_type=f32)


def tn(a, b):
    return lax.dot_general(a, b, (((0,), (0,)), ((), ())), preferred_element_type=f32)


def norm_forward(values, gain):
    inverse = lax.rsqrt(jnp.mean(values * values, axis=-1, keepdims=True) + eps_norm)
    return (values * inverse * gain, inverse)


def norm_backward(values, inverse, gain, grads):
    weighted = grads * gain
    return inverse * weighted - values * (inverse * inverse * inverse) * jnp.mean(
        values * weighted, axis=-1, keepdims=True
    )


def rope_tables():
    half = HEAD_SIZE // 2
    frequency = jnp.exp(
        jnp.arange(half, dtype=f32) * (-2.0 * math.log(rope_base) / HEAD_SIZE)
    )
    position = jnp.arange((PBLK + 1) * BLOCK, dtype=f32)
    angles = position[:, None] * frequency[None, :]
    cosine, sine = jnp.cos(angles), jnp.sin(angles)
    return (
        jnp.concatenate([cosine, cosine], axis=1),
        jnp.concatenate([-sine, sine], axis=1),
    )


def select_matrix(role_row, owner_row):
    matches = (role_row - PBLK)[:, None] == jnp.arange(CONTS, dtype=jnp.int32)[None, :]
    owner_slot = jnp.max(jnp.where(matches, owner_row[None, :], -1), axis=1)
    owner_tok = jnp.repeat(owner_slot, BLOCK)
    column_owner = jnp.arange(RANKS, dtype=jnp.int32) // R
    return (owner_tok[:, None] == column_owner[None, :]).astype(f32)


def half_roll(x):
    return pltpu.roll(x, shift=HEAD_SIZE // 2, axis=1)


def causal_block(heads):
    rows = lax.broadcasted_iota(jnp.int32, (heads * BLOCK, BLOCK), 0) % BLOCK
    cols = lax.broadcasted_iota(jnp.int32, (heads * BLOCK, BLOCK), 1)
    return cols <= rows


def stack_heads(x):
    heads = x.shape[1] // HEAD_SIZE
    return jnp.concatenate(
        [x[:, j * HEAD_SIZE : (j + 1) * HEAD_SIZE] for j in range(heads)], axis=0
    )


def unstack_heads(x):
    heads = x.shape[0] // BLOCK
    return jnp.concatenate([x[j * BLOCK : (j + 1) * BLOCK] for j in range(heads)], axis=1)


def slot_rows(slot_ref, role):
    return pl.ds(pl.multiple_of(slot_ref[role] * BLOCK, BLOCK), BLOCK)


def role_rows(role):
    return pl.ds(pl.multiple_of(role * BLOCK, BLOCK), BLOCK)


def stack_rows(role, heads):
    n = heads * BLOCK
    return pl.ds(pl.multiple_of(role * n, n), n)


def attention_forward_kernel(slot_ref, proj_ref, cos_ref, sin_ref, attn_ref, qs_ref, kv_ref, lse_ref):
    heads = attn_ref.shape[1] // HEAD_SIZE
    qcols = heads * HEAD_SIZE

    def prepare(role, _):
        rows = slot_rows(slot_ref, role)
        table = role_rows(jnp.minimum(role, PBLK))
        cosine, sine = cos_ref[table, :], sin_ref[table, :]

        def turned(c):
            v = proj_ref[rows, c * HEAD_SIZE : (c + 1) * HEAD_SIZE]
            return (v * cosine + half_roll(v) * sine).astype(bf16)

        qs_ref[stack_rows(role, heads), :] = jnp.concatenate(
            [turned(j) for j in range(heads)], axis=0
        )
        kv_ref[role_rows(role), :HEAD_SIZE] = turned(heads)
        kv_ref[role_rows(role), HEAD_SIZE:] = proj_ref[rows, qcols + HEAD_SIZE :].astype(bf16)
        return 0

    lax.fori_loop(0, SLOTS, prepare, 0)
    causal = causal_block(heads)

    def one(role, prompt_blocks, own):
        q = qs_ref[stack_rows(role, heads), :]
        own_k = kv_ref[own, :HEAD_SIZE]
        own_v = kv_ref[own, HEAD_SIZE:]
        s_own = jnp.where(causal, nt(q, own_k) * score_scale, NEG)
        top = jnp.max(s_own, axis=1, keepdims=True)
        if prompt_blocks:
            n = prompt_blocks * BLOCK
            s_pre = nt(q, kv_ref[:n, :HEAD_SIZE]) * score_scale
            top = jnp.maximum(top, jnp.max(s_pre, axis=1, keepdims=True))
        e_own = jnp.exp(s_own - top)
        total = jnp.sum(e_own, axis=1, keepdims=True)
        out = nn(e_own.astype(bf16), own_v)
        if prompt_blocks:
            e_pre = jnp.exp(s_pre - top)
            total = total + jnp.sum(e_pre, axis=1, keepdims=True)
            out = out + nn(e_pre.astype(bf16), kv_ref[:n, HEAD_SIZE:])
        out = out / total
        lse_ref[stack_rows(role, heads), :] = top + jnp.log(total)
        attn_ref[slot_rows(slot_ref, role), :] = unstack_heads(out).astype(bf16)

    for role in range(PBLK):
        one(role, role, slice(role * BLOCK, (role + 1) * BLOCK))

    def later(c, _):
        one(PBLK + c, PBLK, role_rows(PBLK + c))
        return 0

    lax.fori_loop(0, CONTS, later, 0)


def attention_forward(slots, projected, cosine, sine):
    tokens = projected.shape[0]
    heads = projected.shape[1] // HEAD_SIZE - 2
    vm = pl.BlockSpec(memory_space=pltpu.VMEM)
    return pl.pallas_call(
        attention_forward_kernel,
        out_shape=(
            jax.ShapeDtypeStruct((tokens, heads * HEAD_SIZE), bf16),
            jax.ShapeDtypeStruct((tokens * heads, HEAD_SIZE), bf16),
            jax.ShapeDtypeStruct((tokens, 2 * HEAD_SIZE), bf16),
            jax.ShapeDtypeStruct((tokens * heads, 1), f32),
        ),
        in_specs=[pl.BlockSpec(memory_space=pltpu.SMEM), vm, vm, vm],
        out_specs=(vm, vm, vm, vm),
        cost_estimate=pl.CostEstimate(
            flops=4 * 10**9, bytes_accessed=10 * 2**20, transcendentals=4 * 10**6
        ),
        name="attention_forward",
    )(slots, projected, cosine, sine)


def attention_backward_kernel(
    slot_ref, qs_ref, kv_ref, lse_ref, grad_ref, cos_ref, sin_ref, out_ref, dk_ref, dv_ref
):
    heads = grad_ref.shape[1] // HEAD_SIZE
    qcols = heads * HEAD_SIZE
    dk_ref[...] = jnp.zeros_like(dk_ref)
    dv_ref[...] = jnp.zeros_like(dv_ref)
    causal = causal_block(heads)

    def turned_back(g, role):
        table = role_rows(jnp.minimum(role, PBLK))
        return g * cos_ref[table, :] - half_roll(g) * sin_ref[table, :]

    def one(role, prompt_blocks, own):
        q = qs_ref[stack_rows(role, heads), :]
        lse = lse_ref[stack_rows(role, heads), :]
        rows = slot_rows(slot_ref, role)
        g = stack_heads(grad_ref[rows, :])
        own_k = kv_ref[own, :HEAD_SIZE]
        own_v = kv_ref[own, HEAD_SIZE:]
        p_own = jnp.exp(jnp.where(causal, nt(q, own_k) * score_scale, NEG) - lse)
        dp_own = nt(g, own_v)
        centre = jnp.sum(p_own * dp_own, axis=1, keepdims=True)
        if prompt_blocks:
            n = prompt_blocks * BLOCK
            pre_k = kv_ref[:n, :HEAD_SIZE]
            p_pre = jnp.exp(nt(q, pre_k) * score_scale - lse)
            dp_pre = nt(g, kv_ref[:n, HEAD_SIZE:])
            centre = centre + jnp.sum(p_pre * dp_pre, axis=1, keepdims=True)
        ds_own = (p_own * (dp_own - centre) * score_scale).astype(bf16)
        dq = nn(ds_own, own_k)
        dk_ref[own, :] += tn(ds_own, q)
        dv_ref[own, :] += tn(p_own.astype(bf16), g)
        if prompt_blocks:
            ds_pre = (p_pre * (dp_pre - centre) * score_scale).astype(bf16)
            dq = dq + nn(ds_pre, pre_k)
            dk_ref[:n, :] += tn(ds_pre, q)
            dv_ref[:n, :] += tn(p_pre.astype(bf16), g)
        for j in range(heads):
            out_ref[rows, j * HEAD_SIZE : (j + 1) * HEAD_SIZE] = turned_back(
                dq[j * BLOCK : (j + 1) * BLOCK], role
            ).astype(bf16)

    for role in range(PBLK):
        one(role, role, slice(role * BLOCK, (role + 1) * BLOCK))

    def later(c, _):
        one(PBLK + c, PBLK, role_rows(PBLK + c))
        return 0

    lax.fori_loop(0, CONTS, later, 0)

    def finish(role, _):
        rows = slot_rows(slot_ref, role)
        out_ref[rows, qcols : qcols + HEAD_SIZE] = turned_back(dk_ref[role_rows(role), :], role).astype(bf16)
        out_ref[rows, qcols + HEAD_SIZE :] = dv_ref[role_rows(role), :].astype(bf16)
        return 0

    lax.fori_loop(0, SLOTS, finish, 0)


def attention_backward(slots, qs, kv, lse, grad, cosine, sine):
    tokens = kv.shape[0]
    vm = pl.BlockSpec(memory_space=pltpu.VMEM)
    return pl.pallas_call(
        attention_backward_kernel,
        out_shape=jax.ShapeDtypeStruct((tokens, grad.shape[1] + 2 * HEAD_SIZE), bf16),
        in_specs=[pl.BlockSpec(memory_space=pltpu.SMEM)] + [vm] * 6,
        out_specs=vm,
        scratch_shapes=[
            pltpu.VMEM((tokens, HEAD_SIZE), f32),
            pltpu.VMEM((tokens, HEAD_SIZE), f32),
        ],
        cost_estimate=pl.CostEstimate(
            flops=9 * 10**9, bytes_accessed=10 * 2**20, transcendentals=4 * 10**6
        ),
        name="attention_backward",
    )(slots, qs, kv, lse, grad, cosine, sine)


PLANE = 8


def neighbours():
    me = lax.axis_index("seq")
    core, x, y = me % 2, (me // 2) % 2, me // 4
    p = me + 1 - 2 * core
    nx = me + 2 - 4 * x
    ny = me + 4 - 8 * y
    nd = nx + 4 - 8 * y
    return me, p, nx, ny, nd


def across(i):
    return i + 1 - 2 * (i % 2)


def greet(*others):
    barrier = pltpu.get_barrier_semaphore()
    for other in others:
        pl.semaphore_signal(
            barrier, inc=1, device_id={"seq": other}, device_id_type=pl.DeviceIdType.MESH
        )
    pl.semaphore_wait(barrier, len(others))


class Links:
    def __init__(self, send_sem, recv_sem):
        self.send_sem, self.recv_sem, self.made = send_sem, recv_sem, {}

    def start(self, k, src, dst, to):
        copy = pltpu.make_async_remote_copy(
            src_ref=src,
            dst_ref=dst,
            send_sem=self.send_sem.at[k],
            recv_sem=self.recv_sem.at[k],
            device_id={"seq": to},
            device_id_type=pl.DeviceIdType.MESH,
        )
        copy.start()
        self.made[k] = copy

    def arrived(self, k):
        self.made[k].wait_recv()

    def drain(self):
        for copy in self.made.values():
            copy.wait_send()


def gather_kernel(count, *refs):
    own_refs, all_refs = refs[:count], refs[count : 2 * count]
    send_sem, recv_sem = refs[2 * count :]
    own = own_refs[0].shape[0]
    half = own // 2
    me, p, nx, ny, nd = neighbours()
    greet(p, nx, ny)
    links = Links(send_sem, recv_sem)
    arrays = range(count)

    def piece(j, i, h):
        return all_refs[j].at[pl.ds(pl.multiple_of(i * own + h * half, half), half), :]

    def mine(j, h):
        return own_refs[j].at[h * half : (h + 1) * half, :]

    def block(j):
        return all_refs[j].at[pl.ds(pl.multiple_of(me * own, own), own), :]

    def each(k, copy):
        for j in arrays:
            links.start(13 * j + k, *copy(j))

    def arrived(k):
        for j in arrays:
            links.arrived(13 * j + k)

    each(0, lambda j: (mine(j, 0), piece(j, me, 0), nx))
    each(1, lambda j: (mine(j, 1), piece(j, me, 1), ny))
    each(2, lambda j: (mine(j, 1), piece(j, me, 1), nx))
    each(3, lambda j: (mine(j, 0), piece(j, me, 0), ny))
    each(4, lambda j: (own_refs[j], block(j), p))
    for j in arrays:
        all_refs[j][pl.ds(pl.multiple_of(me * own, own), own), :] = own_refs[j][...]

    def pass_on(k, i, h, to):
        each(k, lambda j: (piece(j, i, h), piece(j, i, h), to))

    arrived(0)
    pass_on(5, nx, 0, ny)
    pass_on(7, nx, 0, p)
    arrived(1)
    pass_on(6, ny, 1, nx)
    pass_on(8, ny, 1, p)
    arrived(2)
    pass_on(9, nx, 1, p)
    arrived(3)
    pass_on(10, ny, 0, p)
    arrived(5)
    pass_on(11, nd, 0, p)
    arrived(6)
    pass_on(12, nd, 1, p)
    for k in (4, 7, 8, 9, 10, 11, 12):
        arrived(k)
    links.drain()


def gather_tokens(collective_id, *arrays):
    if lax.axis_size("seq") != PLANE:
        return tuple(lax.all_gather(x, "seq", axis=0, tiled=True) for x in arrays)
    vm = pl.BlockSpec(memory_space=pltpu.VMEM)
    count = len(arrays)
    size = sum(x.shape[0] * x.shape[1] for x in arrays)
    return pl.pallas_call(
        functools.partial(gather_kernel, count),
        out_shape=tuple(
            jax.ShapeDtypeStruct((PLANE * x.shape[0], x.shape[1]), x.dtype) for x in arrays
        ),
        in_specs=[vm] * count,
        out_specs=(vm,) * count,
        scratch_shapes=[
            pltpu.SemaphoreType.DMA((13 * count,)),
            pltpu.SemaphoreType.DMA((13 * count,)),
        ],
        compiler_params=pltpu.CompilerParams(collective_id=collective_id, has_side_effects=True),
        cost_estimate=pl.CostEstimate(
            flops=0, bytes_accessed=10 * PLANE * size, transcendentals=0
        ),
    )(*arrays)


COLS = 256


def scatter_kernel(modes, rank_from, count, *refs):
    n, m = len(modes), len(rank_from)
    a_refs, b_refs, r_refs = refs[:count], refs[count : count + n], refs[count + n : count + n + m]
    refs = refs[count + n + m :]
    out_ref, rank_ref = (refs[0], refs[1]) if m else (refs[0], None)
    theirs, cores, sums, relay, last, send_sem, recv_sem = refs[2 if m else 1 :]
    own, width = out_ref.shape
    half = own // 2
    per = RANKS
    ranks = m * per
    me, p, nx, ny, nd = neighbours()
    greet(p, nx, ny)
    links = Links(send_sem, recv_sem)

    def product(i, store):
        rows = pl.ds(pl.multiple_of(i * own, own), own)

        def tile(t, _):
            cols = pl.ds(pl.multiple_of(t * COLS, COLS), COLS)
            total = None
            for a, b, transposed in zip(a_refs, b_refs, modes):
                term = nt(a[rows, :], b[cols, :]) if transposed else nn(a[rows, :], b[:, cols])
                total = term if total is None else total + term
            store(cols, total)
            return 0

        lax.fori_loop(0, width // COLS, tile, 0)
        for j, r in enumerate(r_refs):
            product = nt(a_refs[rank_from[j]][rows, :], r[...])
            store(slice(width + j * per, width + (j + 1) * per), product)

    def for_partner(slot, i):
        def store(cols, value):
            theirs[slot, :, cols] = value.astype(bf16)

        product(across(i), store)
        links.start(slot, theirs.at[slot], cores.at[slot], p)

    def chip_sum(slot, i):
        def store(cols, value):
            sums[slot, :, cols] = (value + cores[slot, :, cols].astype(f32)).astype(bf16)

        product(i, store)

    for_partner(0, nd)
    for_partner(1, nx)
    links.arrived(0)
    chip_sum(0, nd)
    links.start(4, sums.at[0, :half], relay.at[0], nx)
    links.start(5, sums.at[0, half:], relay.at[1], ny)
    links.arrived(1)
    chip_sum(1, nx)
    links.start(6, sums.at[1, :half], last.at[0, :half], nx)
    for_partner(2, ny)
    for_partner(3, me)
    links.arrived(2)
    chip_sum(2, ny)
    links.start(7, sums.at[2, half:], last.at[1, half:], ny)
    links.arrived(5)
    sums[1, half:, :] = (sums[1, half:, :].astype(f32) + relay[1].astype(f32)).astype(bf16)
    links.start(8, sums.at[1, half:], last.at[0, half:], nx)
    links.arrived(4)
    sums[2, :half, :] = (sums[2, :half, :].astype(f32) + relay[0].astype(f32)).astype(bf16)
    links.start(9, sums.at[2, :half], last.at[1, :half], ny)
    links.arrived(3)

    def keep(cols, value):
        value = value + cores[3, :, cols].astype(f32)
        if isinstance(cols, slice):
            rank_ref[:, cols.start - width : cols.stop - width] = value
        else:
            out_ref[:, cols] = value

    product(me, keep)
    for k in (6, 7, 8, 9):
        links.arrived(k)
    both = lambda cols: last[0, :, cols].astype(f32) + last[1, :, cols].astype(f32)
    out_ref[...] = out_ref[...] + both(slice(0, width))
    if m:
        rank_ref[...] = rank_ref[...] + both(slice(width, width + ranks))
    links.drain()


def scatter_products(a, b, modes, rank_maps, rank_from, collective_id):
    width = b[0].shape[0] if modes[0] else b[0].shape[1]
    ranks = RANKS * len(rank_maps)
    seq = lax.axis_size("seq")
    rows = a[0].shape[0]
    own = rows // seq
    if seq != PLANE:
        total = sum(nt(x, y) if m else nn(x, y) for x, y, m in zip(a, b, modes))
        extra = [nt(a[i], y) for i, y in zip(rank_from, rank_maps)]
        both = jnp.concatenate([total] + extra, axis=1).astype(bf16)
        both = lax.psum_scatter(both, "seq", scatter_dimension=0, tiled=True).astype(f32)
        return both[:, :width], both[:, width:]
    vm = pl.BlockSpec(memory_space=pltpu.VMEM)
    whole = width + ranks
    depth = sum(x.shape[1] for x in a)
    shapes = [jax.ShapeDtypeStruct((own, width), f32)]
    if ranks:
        shapes.append(jax.ShapeDtypeStruct((own, ranks), f32))
    out = pl.pallas_call(
        functools.partial(scatter_kernel, tuple(modes), tuple(rank_from), len(a)),
        out_shape=tuple(shapes),
        in_specs=[vm] * (len(a) + len(b) + len(rank_maps)),
        out_specs=(vm,) * len(shapes),
        scratch_shapes=[
            pltpu.VMEM((4, own, whole), bf16),
            pltpu.VMEM((4, own, whole), bf16),
            pltpu.VMEM((3, own, whole), bf16),
            pltpu.VMEM((2, own // 2, whole), bf16),
            pltpu.VMEM((2, own, whole), bf16),
            pltpu.SemaphoreType.DMA((10,)),
            pltpu.SemaphoreType.DMA((10,)),
        ],
        compiler_params=pltpu.CompilerParams(collective_id=collective_id, has_side_effects=True),
        cost_estimate=pl.CostEstimate(
            flops=2 * rows * depth * whole + 4 * 10**10,
            bytes_accessed=rows * depth * 4,
            transcendentals=0,
        ),
    )(*a, *b, *rank_maps)
    return (out[0], out[1]) if ranks else (out[0], None)


def head_columns(w, seq):
    split = seq // KEY_VALUE_HEADS
    if split == 1:
        return w
    rows, own = w.shape[0], HEADS_PER_GROUP // split
    w = w.reshape(rows, KEY_VALUE_HEADS, HEADS_PER_GROUP + 2, HEAD_SIZE)
    q = w[:, :, :HEADS_PER_GROUP].reshape(rows, KEY_VALUE_HEADS, split, own, HEAD_SIZE)
    kv = jnp.broadcast_to(
        w[:, :, None, HEADS_PER_GROUP:], (rows, KEY_VALUE_HEADS, split, 2, HEAD_SIZE)
    )
    return jnp.concatenate([q, kv], axis=3).reshape(rows, -1)


def joined_grad(g, seq):
    split = seq // KEY_VALUE_HEADS
    if split == 1:
        return g
    own = HEADS_PER_GROUP // split
    lead = g.shape[:-1]
    g = g.reshape(*lead, KEY_VALUE_HEADS, split, own + 2, HEAD_SIZE)
    q = g[..., :own, :].reshape(*lead, KEY_VALUE_HEADS, HEADS_PER_GROUP, HEAD_SIZE)
    return jnp.concatenate([q, jnp.sum(g[..., own:, :], axis=-3)], axis=-2).reshape(*lead, -1)


def exchange_kernel(count, *refs):
    in_refs, out_refs = refs[:count], refs[count : 2 * count]
    send_sem, recv_sem = refs[2 * count :]
    me = lax.axis_index("seq")
    others = [lax.rem(me + k, PLANE) for k in range(1, PLANE)]
    greet(*others)
    links = Links(send_sem, recv_sem)

    def columns(j, i):
        part = in_refs[j].shape[1] // PLANE
        return pl.ds(pl.multiple_of(i * part, part), part)

    for j in range(count):
        for k, other in enumerate(others):
            links.start(
                (PLANE - 1) * j + k, in_refs[j].at[:, columns(j, other)], out_refs[j].at[me], other
            )
    for j in range(count):
        out_refs[j][me] = in_refs[j][:, columns(j, me)]
    for k in range((PLANE - 1) * count):
        links.arrived(k)
    links.drain()


def exchange_columns(collective_id, *arrays):
    seq = lax.axis_size("seq")
    shapes = tuple(
        jax.ShapeDtypeStruct((seq, w.shape[0], w.shape[1] // seq), w.dtype) for w in arrays
    )
    if seq != PLANE:
        return tuple(
            lax.all_to_all(w, "seq", split_axis=1, concat_axis=0, tiled=True).reshape(t.shape)
            for w, t in zip(arrays, shapes)
        )
    vm = pl.BlockSpec(memory_space=pltpu.VMEM)
    count = len(arrays)
    copies = (PLANE - 1) * count
    return pl.pallas_call(
        functools.partial(exchange_kernel, count),
        out_shape=shapes,
        in_specs=[vm] * count,
        out_specs=(vm,) * count,
        scratch_shapes=[
            pltpu.SemaphoreType.DMA((copies,)),
            pltpu.SemaphoreType.DMA((copies,)),
        ],
        compiler_params=pltpu.CompilerParams(collective_id=collective_id, has_side_effects=True),
        cost_estimate=pl.CostEstimate(
            flops=0, bytes_accessed=20 * sum(w.size for w in arrays), transcendentals=0
        ),
    )(*arrays)


def all_rows(part):
    return lax.all_gather(part, "ad", axis=1, tiled=True).reshape(-1, part.shape[2])


def local(
    tokens,
    out_grad,
    block_role,
    adapter_of,
    attn_gain,
    ffn_gain,
    wqkv,
    wo,
    ffn,
    qkv_a,
    qkv_b,
    out_a,
    out_b,
    ffn_in_a,
    ffn_in_b,
    ffn_out_a,
    ffn_out_b,
):
    own = tokens.shape[1]
    width = tokens.shape[2]
    seq = lax.axis_size("seq")
    rank_seq = lax.axis_index("seq")
    ff_part = FF // seq
    wqkv = head_columns(wqkv, seq)
    qkv_part = wqkv.shape[1] // seq
    head_part = QUERY_HEADS * HEAD_SIZE // seq
    row_start = rank_seq * own

    def my_columns(a, part):
        return lax.dynamic_slice_in_dim(a, rank_seq * part, part, a.ndim - 1)

    def stack_ad(a):
        return lax.all_gather(a, "ad", axis=0, tiled=True)

    role_row = block_role[0]
    slots = jnp.argsort(role_row).astype(jnp.int32)
    select_all = select_matrix(role_row, adapter_of[0])
    select_all_b = select_all.astype(bf16)
    select_own = lax.dynamic_slice_in_dim(select_all, row_start, own, 0)
    select_own_b = select_own.astype(bf16)
    cosine, sine = rope_tables()

    flat = lambda a: a.reshape(-1, a.shape[-1])
    whole_maps = [qkv_a, out_b, ffn_in_a[:, 0], ffn_in_a[:, 1], ffn_out_b]
    part_maps = [
        (head_columns(flat(qkv_b), seq), qkv_part),
        (flat(out_a), head_part),
        (flat(ffn_in_b[:, 0]), ff_part),
        (flat(ffn_in_b[:, 1]), ff_part),
        (flat(ffn_out_a), ff_part),
    ]
    wpart = width // seq
    pieces = [my_columns(flat(m), wpart) for m in whole_maps]
    pieces += [my_columns(m, part) for m, part in part_maps]
    pieces.append(wo.reshape(pieces[0].shape[0], -1))
    (qkv_cols,) = exchange_columns(10, wqkv)
    qkv_w = all_rows(qkv_cols)
    together = stack_ad(jnp.concatenate(pieces, axis=1))
    at = len(whole_maps) * wpart
    (spread,) = gather_tokens(7, together[:, :at])
    spread = spread.reshape(seq, RANKS, len(whole_maps), wpart).transpose(2, 1, 0, 3)
    spread = spread.reshape(len(whole_maps), RANKS, width)
    qkv_enter, out_leave, gate_enter, upper_enter, down_leave = (
        spread[k] for k in range(len(whole_maps))
    )
    parts = []
    for _, c in part_maps:
        parts.append(together[:, at : at + c])
        at += c
    qkv_leave, out_enter, gate_leave, upper_leave, down_enter = parts
    out_w = together[:, at:].reshape(-1, width)

    w1, w3, w2 = map(all_rows, exchange_columns(11, ffn[:, 0], ffn[:, 1], ffn[:, 2]))

    inputs_f = tokens[0].astype(f32)
    normed, inverse_attn = norm_forward(inputs_f, attn_gain)
    normed_attn = normed.astype(bf16)
    (normed_attn_all,) = gather_tokens(1, normed_attn)
    rank_qkv = nt(normed_attn_all, qkv_enter).astype(bf16) * select_all_b
    projected = nn(normed_attn_all, qkv_w) + nn(rank_qkv, qkv_leave)
    attn, qs, kv, lse = attention_forward(slots, projected, cosine, sine)
    branch, rank_out = scatter_products([attn], [out_w], [False], [out_enter], [0], 2)
    rank_out = rank_out.astype(bf16) * select_own_b
    residual = inputs_f + branch + nn(rank_out, out_leave)
    normed_two, inverse_ffn = norm_forward(residual, ffn_gain)
    normed_ffn = normed_two.astype(bf16)
    (normed_ffn_all,) = gather_tokens(1, normed_ffn)
    rank_gate = nt(normed_ffn_all, gate_enter).astype(bf16) * select_all_b
    rank_upper = nt(normed_ffn_all, upper_enter).astype(bf16) * select_all_b
    gate_val = nn(normed_ffn_all, w1) + nn(rank_gate, gate_leave)
    upper_val = nn(normed_ffn_all, w3) + nn(rank_upper, upper_leave)
    sigma = jax.nn.sigmoid(gate_val)
    silu_gate = gate_val * sigma
    hidden = (silu_gate * upper_val).astype(bf16)
    grad_down = out_grad[0]
    (grad_all,) = gather_tokens(1, grad_down)
    d_rank_down = (nt(grad_all, down_leave) * select_all).astype(bf16)
    d_hidden = nn(grad_all, w2) + nn(d_rank_down, down_enter)
    d_gate = (d_hidden * upper_val * sigma * (1.0 + gate_val * (1.0 - sigma))).astype(bf16)
    d_upper = (d_hidden * silu_gate).astype(bf16)
    back, back_rank = scatter_products(
        [d_gate, d_upper, hidden],
        [w1, w3],
        [True, True],
        [gate_leave, upper_leave, down_enter],
        [0, 1, 2],
        4,
    )
    d_rank_gate = (back_rank[:, :RANKS] * select_own).astype(bf16)
    d_rank_upper = (back_rank[:, RANKS : 2 * RANKS] * select_own).astype(bf16)
    rank_down = back_rank[:, 2 * RANKS :].astype(bf16) * select_own_b
    d_normed_ffn = back + nn(d_rank_gate, gate_enter) + nn(d_rank_upper, upper_enter)
    d_residual = grad_down.astype(f32) + norm_backward(
        residual, inverse_ffn, ffn_gain, d_normed_ffn
    )
    d_branch = d_residual.astype(bf16)
    ranks_own = jnp.concatenate([rank_out, d_rank_gate, d_rank_upper, rank_down], axis=1)
    d_branch_all, ranks_all = gather_tokens(6, d_branch, ranks_own)
    hidden_late, ranks_all = lax.optimization_barrier((hidden, ranks_all))
    down_part = nt(hidden_late, w2).astype(bf16)
    d_branch_all, down_part = lax.optimization_barrier((d_branch_all, down_part))
    down = lax.psum_scatter(down_part, "seq", scatter_dimension=0, tiled=True).astype(f32)
    d_rank_out = (nt(d_branch_all, out_leave) * select_all).astype(bf16)
    d_attn = (nt(d_branch_all, out_w) + nn(d_rank_out, out_enter)).astype(bf16)
    d_projected = attention_backward(slots, qs, kv, lse, d_attn, cosine, sine)
    back_attn, back_rank_qkv = scatter_products([d_projected], [qkv_w], [True], [qkv_leave], [0], 5)
    d_rank_qkv = (back_rank_qkv * select_own).astype(bf16)
    d_normed_attn = back_attn + nn(d_rank_qkv, qkv_enter)
    input_grad = (d_residual + norm_backward(inputs_f, inverse_attn, attn_gain, d_normed_attn))[
        None
    ]

    def reduced(sums):
        both = jnp.concatenate([x.astype(bf16) for x in sums], axis=1)
        return lax.psum_scatter(both, "ad", scatter_dimension=0, tiled=True)

    def unpack(arr, counts):
        out, at = [], 0
        for c in counts:
            piece = arr[:, :, at : at + c].transpose(1, 0, 2).astype(f32)
            out.append(piece.reshape(piece.shape[0] // R, R, seq * c))
            at += c
        return out

    columns = lambda x: my_columns(x, wpart)
    rank_out_all, d_rank_gate_all, d_rank_upper_all, rank_down_all = (
        ranks_all[:, k * RANKS : (k + 1) * RANKS] for k in range(4)
    )
    normed_columns = columns(normed_ffn_all)
    early = reduced(
        [
            tn(rank_out_all, columns(d_branch_all)),
            tn(d_rank_gate_all, normed_columns),
            tn(d_rank_upper_all, normed_columns),
            tn(rank_down_all, columns(grad_all)),
            tn(d_rank_out, attn),
            tn(rank_gate, d_gate),
            tn(rank_upper, d_upper),
            tn(d_rank_down, hidden),
        ]
    )
    (d_rank_qkv_all,) = gather_tokens(8, d_rank_qkv)
    late_sums = [tn(d_rank_qkv_all, columns(normed_attn_all)), tn(rank_qkv, d_projected)]
    late = reduced(late_sums)
    (grads,) = gather_tokens(9, jnp.concatenate([early, late], axis=1))
    grads = grads.reshape(seq, -1, grads.shape[1])
    g_out_b, g_ia0, g_ia1, g_ob, g_out_a, g_ib0, g_ib1, g_oa, g_qkv_a, g_qkv_b = unpack(
        grads, [wpart] * 4 + [head_part] + [ff_part] * 3 + [wpart, qkv_part]
    )
    output = (residual + down + nn(rank_down, down_leave)).astype(bf16)[None]
    return (
        output,
        input_grad,
        g_qkv_a,
        joined_grad(g_qkv_b, seq),
        g_out_a,
        g_out_b,
        jnp.stack([g_ia0, g_ia1], axis=1),
        jnp.stack([g_ib0, g_ib1], axis=1),
        g_oa,
        g_ob,
    )


def solution(mesh):
    ad3 = P("ad", None, None)
    ad4 = P("ad", None, None, None)
    return jax.shard_map(
        local,
        mesh=mesh,
        in_specs=(
            P("ad", "seq", None),
            P("ad", "seq", None),
            P("ad", None),
            P("ad", None),
            P(),
            P(),
            P(("seq", "ad"), None),
            P(("seq", "ad"), None),
            P(("seq", "ad"), None, None),
            ad3,
            ad3,
            ad3,
            ad3,
            ad4,
            ad4,
            ad3,
            ad3,
        ),
        out_specs=(
            P("ad", "seq", None),
            P("ad", "seq", None),
            ad3,
            ad3,
            ad3,
            ad3,
            ad4,
            ad4,
            ad3,
            ad3,
        ),
        check_vma=False,
    )
```
